32 devices in a mesh: gx: 4 (over z), gy: 4 (over y, x), gz: 2 (over core).
Axes of the slice: x: 2, y: 2, z: 4, core: 2. Of those that a mesh axis runs over, the one named last changes fastest.
Arguments:
- coarse_field: float32 [3, 128, 128, 512], P(None, 'gx', 'gy', 'gz'), may hold values from -6 to 6
- fine_field: float32 [3, 128, 16, 256], P(None, ('gx', 'gy', 'gz')), may hold values from -6 to 6
- viscosity: float32 [128, 16, 256], P(('gx', 'gy', 'gz')), may hold values from 0.1 to 1
- corners: int32 [64, 3], replicated, may hold values from 0 to 504, as said below
- grid_slot: int32 [64], replicated, may hold values from 0 to 127, as said below
- neighbors: int32 [64, 2], replicated, may hold values from -1 to 63, as said below
Outputs:
- fine_out: float32 [3, 128, 16, 256], P(None, ('gx', 'gy', 'gz'))
- coarse_out: float32 [3, 128, 128, 512], P(None, 'gx', 'gy', 'gz')
The draws below stay inside these ranges and needn't reach their ends.
Inputs may be any that keep to these rules, and one draw needn't show every extreme that they name: Each box is 8 coarse cells on a side, its corner coordinates are multiples of 8, it lies inside the domain and inside one coarse brick of 32 x 32 x 256 cells, and different grids have different boxes. A brick holds either no box or exactly 4 boxes, which share their y and z corners and are grids of one wake. `grid_slot`: different grids have different slots. A grid's slot lies on a device with the same gz index as the brick that holds its box. Every device holds at most 4 grids, some device holds 4 grids in every draw, and all grids of one device lie in one brick. `neighbors`: entry 0 is the grid of the same wake whose box touches the grid's lower x face, entry 1 the one touching its upper x face, or -1 where there is none.
All inputs are finite; a program needn't handle non-finite values.
Results may differ from the reference program's by a relative error of at most 0.00005.
Values sent between devices are 32-bit elements; how exact they have to be, the bound alone decides.
A program may use at most 128 MiB of HBM per device.

```python
import math
import jax
import jax.numpy as jnp
from jax import lax

B = 8
F = 16
CY = 32
CZ = 256
SLOTS = 4
WAKE = 8
NX = 128
NY = 128
NZ = 512
N_GX = 4
N_GY = 4
N_GZ = 2


def wind_layout(key):
    root_random_key = jax.random.fold_in(key, 4242)
    groups = N_GX * N_GY
    turbines = groups // 4
    half_x = N_GX // 2
    pair_count = groups // 2
    rows_z = CZ // B
    grid_count = turbines * WAKE
    corner_parts = []
    slot_parts = []
    near_parts = []
    for z_layer in range(N_GZ):
        subkeys = jax.random.split(jax.random.fold_in(root_random_key, z_layer), 7)
        pair_order = jax.random.permutation(subkeys[0], pair_count).astype(jnp.int32)
        first_pair = jax.random.randint(subkeys[1], (), half_x, pair_count, dtype=jnp.int32)
        found_at = jnp.argmax(pair_order == first_pair).astype(jnp.int32)
        pair_order = pair_order.at[found_at].set(pair_order[0]).at[0].set(first_pair)
        chosen = pair_order[:turbines]
        brick_row = chosen // half_x
        brick_first = 2 * (chosen % half_x)
        edge_z = rows_z - 1 if z_layer % 2 == 0 else 0
        inner_y = jax.random.randint(subkeys[2], (turbines,), 0, CY // B, dtype=jnp.int32).at[0].set(0)
        inner_z = jax.random.randint(subkeys[5], (turbines,), 0, rows_z, dtype=jnp.int32).at[0].set(edge_z)
        row_y = brick_row * (CY // B) + inner_y
        row_z = inner_z + z_layer * rows_z
        start_x = brick_first * SLOTS
        along_wake = jnp.arange(WAKE, dtype=jnp.int32)
        lattice_x = (start_x[:, None] + along_wake[None, :]).reshape(-1)
        lattice_y = jnp.repeat(row_y, WAKE)
        lattice_z = jnp.repeat(row_z, WAKE)
        corner_parts.append((jnp.stack([lattice_x, lattice_y, lattice_z], axis=1) * B).astype(jnp.int32))
        local_ids = jnp.arange(grid_count, dtype=jnp.int32)
        global_ids = local_ids + z_layer * grid_count
        in_wake = local_ids % WAKE
        near_parts.append(jnp.stack([jnp.where(in_wake > 0, global_ids - 1, -1), jnp.where(in_wake < WAKE - 1, global_ids + 1, -1)], axis=1).astype(jnp.int32))
        devices = jax.random.permutation(subkeys[3], groups).astype(jnp.int32)
        across = (devices[0] + groups // 2) % groups
        across_at = jnp.argmax(devices == across).astype(jnp.int32)
        devices = devices.at[across_at].set(devices[2]).at[2].set(across)
        second_share = jax.random.randint(subkeys[6], (), 1, SLOTS + 1, dtype=jnp.int32)
        shares = jax.random.randint(subkeys[4], (groups // 2,), 0, SLOTS + 1, dtype=jnp.int32).at[0].set(SLOTS).at[1].set(second_share)
        half_id = local_ids // SLOTS
        inside = local_ids % SLOTS
        share_limit = shares[half_id]
        owner_group = jnp.where(inside < share_limit, devices[2 * half_id], devices[2 * half_id + 1])
        owner_slot = jnp.where(inside < share_limit, inside, inside - share_limit)
        slot_parts.append(((owner_group * N_GZ + z_layer) * SLOTS + owner_slot).astype(jnp.int32))
    corner_table = jnp.concatenate(corner_parts, axis=0)
    slot_table = jnp.concatenate(slot_parts, axis=0)
    near_all = jnp.concatenate(near_parts, axis=0)
    total_count = corner_table.shape[0]
    renumbered_slots = jax.random.permutation(jax.random.fold_in(root_random_key, 777), total_count).astype(jnp.int32)
    inverse_permutation = jnp.argsort(renumbered_slots).astype(jnp.int32)
    mapped_neighbor_slots = jnp.where(near_all >= 0, inverse_permutation[jnp.maximum(near_all, 0)], -1).astype(jnp.int32)
    return (corner_table[renumbered_slots], slot_table[renumbered_slots], mapped_neighbor_slots[renumbered_slots])


def draw_corners(key, part):
    return wind_layout(key)[0]


def draw_grid_slot(key, part):
    return wind_layout(key)[1]


def draw_neighbors(key, part):
    return wind_layout(key)[2]


def steps_of(key, dims, pieces, least, high):
    def one(axis_at, shards_of):
        heights = jax.random.uniform(jax.random.fold_in(jax.random.fold_in(key, 6), axis_at), (shards_of,), jnp.float32, least / len(pieces), high / len(pieces))
        return jnp.repeat(jnp.exp(heights), dims[axis_at] // shards_of).reshape((-1,) + (1,) * (len(dims) - axis_at - 1))

    factor_of = one(*pieces[0])
    for cut in pieces[1:]:
        factor_of = factor_of * one(*cut)
    return factor_of


def centred(own_key, shape, scale, reach, pieces=(), held_as=jnp.bfloat16):
    result = scale * jax.random.normal(own_key, shape, jnp.float32)
    if pieces:
        result = result * steps_of(own_key, shape, pieces, -0.22, 0.18)
    return jnp.clip(result, -reach, reach).astype(held_as)


def setup_inputs(seed: int = 0) -> dict:
    keys = jax.random.split(jax.random.key(seed), 7)
    return {
        "coarse_field": centred(keys[0], (3, NX, NY, NZ), 1.0, 6.0, ((1, 4), (2, 4), (3, 2)), jnp.float32),
        "fine_field": centred(keys[1], (3, N_GX * N_GY * N_GZ * SLOTS, F, F * F), 1.0, 6.0, ((1, 32),), jnp.float32),
        "viscosity": jnp.clip(jnp.exp(math.log(1.0) - 2.3025851 * jax.random.uniform(keys[2], (N_GX * N_GY * N_GZ * SLOTS, F, F * F), jnp.float32) ** steps_of(keys[2], (N_GX * N_GY * N_GZ * SLOTS, F, F * F), ((0, 32),), -0.2, 0.2)), 0.1, 1.0),
        "corners": draw_corners(jax.random.fold_in(keys[6], 71), 0),
        "grid_slot": draw_grid_slot(jax.random.fold_in(keys[6], 71), 0),
        "neighbors": draw_neighbors(jax.random.fold_in(keys[6], 71), 0),
    }


step_rate = 0.15


def tables():
    side = B + 2
    fine_index = jnp.arange(F, dtype=jnp.int32)
    coarse_index = jnp.arange(side, dtype=jnp.int32)
    center = fine_index // 2 + 1
    other = jnp.where(fine_index % 2 == 0, center - 1, center + 1)
    tangent = 0.75 * (coarse_index[None, :] == center[:, None]).astype(jnp.float32) + 0.25 * (coarse_index[None, :] == other[:, None]).astype(jnp.float32)
    low_side = 0.75 * (coarse_index == 0).astype(jnp.float32) + 0.25 * (coarse_index == 1).astype(jnp.float32)
    high_side = 0.75 * (coarse_index == side - 1).astype(jnp.float32) + 0.25 * (coarse_index == side - 2).astype(jnp.float32)
    return tangent, low_side, high_side


def advance(volume, visc_cells, ghost_faces, lower_plane, upper_plane):
    components = volume.shape[0]
    slots_here = volume.shape[1]
    cells_edge = volume.shape[2]
    plane_size = volume.shape[3]
    lane_ids = jnp.arange(plane_size, dtype=jnp.int32)
    lane_y = lane_ids // cells_edge
    lane_z = lane_ids % cells_edge
    x_minus = jnp.concatenate([lower_plane[:, :, None], volume[:, :, :-1]], axis=2)
    x_plus = jnp.concatenate([volume[:, :, 1:], upper_plane[:, :, None]], axis=2)
    shape_four = (components, slots_here, cells_edge, cells_edge)
    y_low = jnp.tile(ghost_faces[:, :, 2].reshape(shape_four), (1, 1, 1, cells_edge))
    y_high = jnp.tile(ghost_faces[:, :, 3].reshape(shape_four), (1, 1, 1, cells_edge))
    z_low = jnp.repeat(ghost_faces[:, :, 4].reshape(shape_four), cells_edge, axis=3)
    z_high = jnp.repeat(ghost_faces[:, :, 5].reshape(shape_four), cells_edge, axis=3)
    zero_row = jnp.zeros_like(volume[..., :cells_edge])
    zero_cell = jnp.zeros_like(volume[..., :1])
    y_minus = jnp.where(lane_y == 0, y_low, jnp.concatenate([zero_row, volume[..., :-cells_edge]], axis=-1))
    y_plus = jnp.where(lane_y == cells_edge - 1, y_high, jnp.concatenate([volume[..., cells_edge:], zero_row], axis=-1))
    z_minus = jnp.where(lane_z == 0, z_low, jnp.concatenate([zero_cell, volume[..., :-1]], axis=-1))
    z_plus = jnp.where(lane_z == cells_edge - 1, z_high, jnp.concatenate([volume[..., 1:], zero_cell], axis=-1))
    neighbor_sum = x_minus + x_plus + y_minus + y_plus + z_minus + z_plus - 6.0 * volume
    return volume + step_rate * visc_cells[None] * neighbor_sum


def reference(coarse_field, fine_field, viscosity, corners, grid_slot, neighbors):
    slot_total = fine_field.shape[1]
    grid_total = corners.shape[0]
    grid_ids = jnp.arange(grid_total, dtype=jnp.int32)
    slot_ids = jnp.arange(slot_total, dtype=jnp.int32)
    slot_match = grid_slot[None, :] == slot_ids[:, None]
    slot_active = jnp.any(slot_match, axis=1)
    slot_grid = jnp.sum(jnp.where(slot_match, grid_ids[None, :], 0), axis=1).astype(jnp.int32)
    box_corner = corners[slot_grid].astype(jnp.int32)
    padded = jnp.pad(coarse_field, ((0, 0), (1, 1), (1, 1), (1, 1)))
    zero_start = jnp.zeros((), jnp.int32)

    def cut_cube(corner):
        return lax.dynamic_slice(padded, (zero_start, corner[0], corner[1], corner[2]), (3, B + 2, B + 2, B + 2))

    cubes = jax.vmap(cut_cube)(box_corner)
    tangent, low_side, high_side = tables()
    highest = lax.Precision.HIGHEST
    face_list = [
        jnp.einsum('nkabc,a,sb,tc->knst', cubes, low_side, tangent, tangent, precision=highest),
        jnp.einsum('nkabc,a,sb,tc->knst', cubes, high_side, tangent, tangent, precision=highest),
        jnp.einsum('nkabc,sa,b,tc->knst', cubes, tangent, low_side, tangent, precision=highest),
        jnp.einsum('nkabc,sa,b,tc->knst', cubes, tangent, high_side, tangent, precision=highest),
        jnp.einsum('nkabc,sa,tb,c->knst', cubes, tangent, tangent, low_side, precision=highest),
        jnp.einsum('nkabc,sa,tb,c->knst', cubes, tangent, tangent, high_side, precision=highest),
    ]
    ghost_faces = jnp.stack([face.reshape(3, slot_total, F * F) for face in face_list], axis=2)
    near_grid = neighbors[slot_grid]
    near_slot = grid_slot[jnp.maximum(near_grid, 0)]
    from_low = fine_field[:, near_slot[:, 0], F - 1, :]
    from_high = fine_field[:, near_slot[:, 1], 0, :]
    has_near = (near_grid >= 0) & slot_active[:, None]
    lower_plane = jnp.where(has_near[None, :, 0, None], from_low, ghost_faces[:, :, 0])
    upper_plane = jnp.where(has_near[None, :, 1, None], from_high, ghost_faces[:, :, 1])
    advanced = advance(fine_field, viscosity, ghost_faces, lower_plane, upper_plane)
    fine_out = jnp.where(slot_active[None, :, None, None], advanced, 0.0)
    averages = advanced.reshape(3, slot_total, B, 2, B, 2, B, 2).mean(axis=(3, 5, 7))

    def place_box(index, field_now):
        corner = box_corner[index]
        start = (zero_start, corner[0], corner[1], corner[2])
        current = lax.dynamic_slice(field_now, start, (3, B, B, B))
        value = jnp.where(slot_active[index], averages[:, index], current)
        return lax.dynamic_update_slice(field_now, value, start)

    coarse_out = lax.fori_loop(0, slot_total, place_box, coarse_field)
    return fine_out, coarse_out
```

```python
import functools
import numpy as np
import jax
import jax.numpy as jnp
from jax import lax
from jax.experimental import pallas as pl
from jax.experimental.pallas import tpu as pltpu
from jax.sharding import PartitionSpec as P

B = 8
F = 16
SLOTS = 4
SIDE = B + 2
LANES = 128
WIDE = 4 * SIDE
IFACES = SLOTS + 1
PLANE_ROWS = 16
A_ROWS = 48
Y_ROWS = 24
E_ROWS = 40
MEAN_ROWS = 12
step_rate = 0.15
MIB = 1 << 20


def tables():
    tangent = np.zeros((F, SIDE), np.float32)
    for f in range(F):
        c = f // 2 + 1
        tangent[f, c] = 0.75
        tangent[f, c - 1 if f % 2 == 0 else c + 1] = 0.25
    low = np.zeros((SIDE,), np.float32)
    low[0], low[1] = 0.75, 0.25
    return tangent, low, low[::-1].copy()


def matrices():
    tangent, low, high = tables()
    eye = np.eye(SIDE, dtype=np.float32)
    cut = np.zeros((SIDE, SIDE, 4, SIDE), np.float32)
    cut[:, :, 0] = np.einsum("b,cd->bcd", low, eye)
    cut[:, :, 1] = np.einsum("b,cd->bcd", high, eye)
    cut[:, :, 2] = np.einsum("bd,c->bcd", eye, low)
    cut[:, :, 3] = np.einsum("bd,c->bcd", eye, high)
    put = np.zeros((4, SIDE, F, F), np.float32)
    put[0, :, 0, :] = tangent.T
    put[1, :, F - 1, :] = tangent.T
    put[2, :, :, 0] = tangent.T
    put[3, :, :, F - 1] = tangent.T
    columns = np.zeros((3, LANES, LANES), np.float32)
    lines = np.zeros((LANES, 8, LANES), np.float32)
    ghost = np.zeros((LANES, 4, F * F), np.float32)
    for k in range(3):
        columns[k, : SIDE * SIDE, k * WIDE : (k + 1) * WIDE] = cut.reshape(SIDE * SIDE, WIDE)
        ghost[k * WIDE : (k + 1) * WIDE, k] = put.reshape(WIDE, F * F)
        for half in range(2):
            for side in range(2):
                for c in range(SIDE):
                    lane = half * 64 + k * 2 * SIDE + side * SIDE + c
                    window = side * (SIDE - 1) * SIDE + c
                    lines[lane, half] = columns[k, window]
                    lines[lane, 2 + 2 * k + half, window] = 1.0
    ghost[: SIDE * SIDE, 3] = np.einsum("sb,tc->bcst", tangent, tangent).reshape(SIDE * SIDE, F * F)
    mean = np.zeros((F * F, LANES), np.float32)
    for y in range(F):
        for z in range(F):
            for half in range(2):
                mean[y * F + z, half * 64 + (y // 2) * B + z // 2] = 0.125
    bf = jnp.bfloat16
    return (
        jnp.asarray(columns.reshape(3 * LANES, LANES), bf),
        jnp.asarray(lines.reshape(LANES, 8 * LANES), bf),
        jnp.asarray(ghost.reshape(LANES, 4 * F * F), bf),
        jnp.asarray(mean, bf),
    )


def div(a, n):
    return lax.div(a, jnp.full_like(a, n))


def rem(a, n):
    return lax.rem(a, jnp.full_like(a, n))


def split(a):
    high = a.astype(jnp.bfloat16)
    return high, (a - high.astype(jnp.float32)).astype(jnp.bfloat16)


def dot(a, b):
    return jnp.dot(a, b, preferred_element_type=jnp.float32)


def exact_right(a, b):
    high, low = split(a)
    return dot(high, b) + dot(low, b)


def exact_left(a, b):
    a = a.astype(jnp.bfloat16)
    high, low = split(b)
    return dot(a, high) + dot(a, low)


def pick(mask, value):
    return jnp.max(jnp.where(mask, value, -1))


def as_float(cond):
    return jnp.where(cond, 1.0, 0.0).astype(jnp.float32)


def grid_tables(bricks, ny, nz, corners, slot_ref):
    x, y, z = corners[0:1, :], corners[1:2, :], corners[2:3, :]
    slot = slot_ref[...]
    brick = (div(x, bricks[0]) * ny + div(y, bricks[1])) * nz + div(z, bricks[2])
    place = rem(y, bricks[1]) * bricks[2] + rem(z, bricks[2])
    return x, y, slot, brick, place


def step_kernel(
    dims, corners_in, slot_in, near_in, coarse, fine_in, visc_in, columns_in, lines_in, ghost_in, mean_in,
    fine_out, picked,
    corners, slot_ref, near_ref, field, fine, visc, columns, lines, ghost, mean,
    window, z_send_a, z_send_y, z_recv_a, z_recv_y, a_buf, y_buf, p1_buf, p2_send, p2_buf, e_send, e_buf,
    advs, m_send, m_buf, q_send, q_buf,
    local_sem, z_sem, y_send_sem, y_recv_sem, x_send_sem, x_recv_sem,
):
    nx, ny, nz, bx, by, bz = dims
    ix, iy, iz = lax.axis_index("gx"), lax.axis_index("gy"), lax.axis_index("gz")
    me = (ix * ny + iy) * nz + iz
    mesh_id = pl.DeviceIdType.MESH

    def local(i, src, dst):
        return pltpu.make_async_copy(src, dst, local_sem.at[i])

    tiles = bz // LANES
    field_loads = [
        local(6 + t, coarse.at[:, t * LANES : (t + 1) * LANES], field.at[t]) for t in range(tiles)
    ]
    loads = [
        local(0, fine_in, fine), local(1, columns_in, columns), local(2, visc_in, visc),
        local(3, lines_in, lines), local(4, ghost_in, ghost), local(5, mean_in, mean),
    ]
    fine_load, columns_load, visc_load, lines_load, ghost_load, mean_load = loads
    first = 6 + tiles
    table_loads = [
        local(first, corners_in, corners), local(first + 1, slot_in, slot_ref), local(first + 2, near_in, near_ref)
    ]
    for load in table_loads + [fine_load] + field_loads + loads[1:]:
        load.start()

    def y_peer(o):
        return lax.rem(iy + o, ny)

    def x_peer(o):
        return lax.rem(ix + o, nx)

    barrier = pltpu.get_barrier_semaphore()
    pl.semaphore_signal(barrier, inc=1, device_id={"gz": 1 - iz}, device_id_type=mesh_id)

    def greet_y(o, c):
        pl.semaphore_signal(barrier, inc=1, device_id={"gy": y_peer(o)}, device_id_type=mesh_id)
        return c

    def greet_x(o, c):
        pl.semaphore_signal(barrier, inc=1, device_id={"gx": x_peer(o)}, device_id_type=mesh_id)
        return c

    lax.fori_loop(1, ny, greet_y, 0)
    lax.fori_loop(1, nx, greet_x, 0)

    def y_copy(which, o, src, dst):
        return pltpu.make_async_remote_copy(
            src_ref=src, dst_ref=dst, send_sem=y_send_sem.at[which, o], recv_sem=y_recv_sem.at[which, o],
            device_id={"gy": y_peer(o)}, device_id_type=mesh_id,
        )

    def x_copy(which, o, src, dst):
        return pltpu.make_async_remote_copy(
            src_ref=src, dst_ref=dst, send_sem=x_send_sem.at[which, o], recv_sem=x_recv_sem.at[which, o],
            device_id={"gx": x_peer(o)}, device_id_type=mesh_id,
        )

    def z_copy(which, src, dst):
        return pltpu.make_async_remote_copy(
            src_ref=src, dst_ref=dst, send_sem=z_sem.at[0, which], recv_sem=z_sem.at[1, which],
            device_id={"gz": 1 - iz}, device_id_type=mesh_id,
        )

    def run(count, make, action):
        def body(o, c):
            getattr(make(o), action)()
            return c

        lax.fori_loop(1, count, body, 0)

    for load in table_loads:
        load.wait()
    gx_, gy_, slot, brick, place = grid_tables((bx, by, bz), ny, nz, corners, slot_ref)
    home = div(gx_, bx) * ny + div(gy_, by)
    box = div(rem(gx_, bx), B)
    dev = div(slot, SLOTS)
    count = slot.shape[1]
    g_row = lax.broadcasted_iota(jnp.int32, (count, count), 0)
    g_col = lax.broadcasted_iota(jnp.int32, (count, count), 1)
    slot_col = jnp.max(jnp.where(g_row == g_col, slot, -1), axis=1, keepdims=True)
    near_slot = []
    far_dev = []
    for side in range(2):
        m = jnp.max(jnp.where(g_row == near_ref[side : side + 1, :], slot_col, -1), axis=0, keepdims=True)
        near_slot.append(m)
        d = div(jnp.maximum(m, 0), SLOTS)
        far_dev.append(jnp.where((m >= 0) & (d != dev), d, -1))

    def anchor(ox, oy, gz):
        hx, hy = ix + ox, iy + oy
        inside = (hx >= 0) & (hx < nx) & (hy >= 0) & (hy < ny)
        code = jnp.maximum(pick(brick == jnp.where(inside, (hx * ny + hy) * nz + gz, -5), place), 0)
        return lax.div(code, bz), lax.rem(code, bz)

    mine = dev == me
    own_slot = [pick(mine & (box == j), rem(slot, SLOTS)) for j in range(SLOTS)]

    fine_load.wait()
    for i in range(IFACES):
        for k in range(3):
            if i == 0:
                row = fine[k, jnp.maximum(own_slot[0], 0), 0:1]
            elif i == SLOTS:
                row = fine[k, jnp.maximum(own_slot[SLOTS - 1], 0), F - 1 : F]
            else:
                below = fine[k, jnp.maximum(own_slot[i - 1], 0), F - 1 : F]
                above = fine[k, jnp.maximum(own_slot[i], 0), 0:1]
                row = jnp.where(own_slot[i - 1] >= 0, below, above)
            p1_buf[iy, i * 3 + k : i * 3 + k + 1] = row
    p1_buf[iy, PLANE_ROWS - 1 : PLANE_ROWS] = jnp.zeros((1, F * F), jnp.float32)
    pl.semaphore_wait(barrier, nx + ny - 1)

    def p1_copy(o):
        return y_copy(0, o, p1_buf.at[iy], p1_buf.at[iy])

    run(ny, p1_copy, "start")

    stride = bx * by
    lane1 = lax.broadcasted_iota(jnp.int32, (1, LANES), 1)
    lane_b = div(lane1, SIDE)
    lane_c = rem(lane1, SIDE)
    half_lane = rem(lane1, 64)
    half_c = rem(half_lane, SIDE)
    line_id = div(half_lane, SIDE)

    def lines_at(z, start, size, step):
        z = lax.rem(z - 1 + bz, bz)
        tile, low = lax.div(z, LANES), lax.rem(z, LANES)
        after = lax.rem(tile + 1, tiles)

        def get(t):
            return field[t, pl.ds(start, size, step)] if step > 1 else field[t, pl.ds(start, size)]

        lane = lax.broadcasted_iota(jnp.int32, (size, LANES), 1)
        return jnp.where(lane >= low, get(tile), get(after)), low

    def shifted(z, start, size, step, to):
        value, low = lines_at(z, start, size, step)
        return pltpu.roll(value, lax.rem(to - low + LANES, LANES), 1)

    def z_weight(z, ids, same):
        first, last = z == 0, z == bz - B
        if same:
            return jnp.where(ids == 0, as_float(~first), jnp.where(ids == SIDE - 1, as_float(~last), 1.0))
        first = as_float(first & (iz == 0))
        last = as_float(last & (iz == 1))
        return jnp.where(ids == 0, first, jnp.where(ids == SIDE - 1, last, 0.0))

    def pack(gz, same, a_to, y_to):
        y, z = anchor(0, 0, gz)
        weight = z_weight(z, lane_c, same)
        weight = weight * jnp.where(lane_b == 0, as_float(y > 0), jnp.where(lane_b == SIDE - 1, as_float(y < by - B), 1.0))
        weight = jnp.where(lane1 < SIDE * SIDE, weight, 0.0)
        for k in range(3):
            acc = jnp.zeros((bx, LANES), jnp.float32)
            for b in range(SIDE):
                row = jnp.clip(y - 1 + b, 0, by - 1)
                acc = jnp.where(lane_b == b, shifted(z, k * stride + row, bx, by, SIDE * b), acc)
            window[k, 0:bx] = acc * weight
        for n, ox in enumerate((1, -1)):
            y, z = anchor(ox, 0, gz)
            weight = z_weight(z, lane_c, same)
            weight = weight * jnp.where(
                lane_b == 0, as_float(y > 0), jnp.where(lane_b == SIDE - 1, as_float(y < by - B), 1.0)
            )
            weight = jnp.where(lane1 < SIDE * SIDE, weight, 0.0)
            x = bx - 1 if ox > 0 else 0
            for k in range(3):
                acc = jnp.zeros((1, LANES), jnp.float32)
                for b in range(SIDE):
                    row = jnp.clip(y - 1 + b, 0, by - 1)
                    acc = jnp.where(lane_b == b, shifted(z, k * stride + x * by + row, 1, 1, SIDE * b), acc)
                window[k, bx + n : bx + n + 1] = acc * weight
        total = jnp.zeros((E_ROWS, LANES), jnp.float32)
        for k in range(3):
            total += exact_right(window[k], columns[k * LANES : (k + 1) * LANES])
            for side in range(2):
                at = bx + 2 + 2 * k + side
                inner = 0 if side == 0 else bx - 1
                a_to[at : at + 1] = window[k, inner : inner + 1]
                a_to[at + 6 : at + 7] = window[k, bx + side : bx + side + 1]
        a_to[0 : bx + 2] = total[0 : bx + 2]
        half = bx // 2
        main = jnp.zeros((half, LANES), jnp.float32)
        ends = [jnp.zeros((1, LANES), jnp.float32) for _ in range(2)]
        for side, oy in enumerate((1, -1)):
            row = by - 1 if oy > 0 else 0
            edge = 0 if oy > 0 else by - B
            y, z = anchor(0, oy, gz)
            weight = z_weight(z, half_c, same) * as_float(y == edge)
            for k in range(3):
                to = k * 2 * SIDE + side * SIDE
                for h in range(2):
                    value = shifted(z, k * stride + h * half * by + row, half, by, to + 64 * h)
                    main = jnp.where((line_id == 2 * k + side) & (div(lane1, 64) == h), value * weight, main)
            for n, ox in enumerate((1, -1)):
                y, z = anchor(ox, oy, gz)
                weight = z_weight(z, half_c, same) * as_float(y == edge)
                x = bx - 1 if ox > 0 else 0
                for k in range(3):
                    to = k * 2 * SIDE + side * SIDE
                    value = shifted(z, k * stride + x * by + row, 1, 1, to)
                    ends[n] = jnp.where((line_id == 2 * k + side) & (lane1 < 64), value * weight, ends[n])
        y_to[0:half] = main
        y_to[half : half + 1] = ends[0]
        y_to[half + 1 : half + 2] = ends[1]

    a_own, y_own = a_buf.at[iy], y_buf.at[iy]
    for k in range(3):
        window[k, bx + 2 : E_ROWS] = jnp.zeros((E_ROWS - bx - 2, LANES), jnp.float32)
    for buf in (z_send_a, a_own):
        buf[bx + 14 : A_ROWS] = jnp.zeros((A_ROWS - bx - 14, LANES), jnp.float32)
    for buf in (z_send_y, y_own):
        buf[bx // 2 + 2 : Y_ROWS] = jnp.zeros((Y_ROWS - bx // 2 - 2, LANES), jnp.float32)
    for load in field_loads:
        load.wait()
    columns_load.wait()
    pack(1 - iz, False, z_send_a, z_send_y)
    to_partner = [z_copy(0, z_send_a, z_recv_a), z_copy(1, z_send_y, z_recv_y)]
    for c in to_partner:
        c.start()
    pack(iz, True, a_own, y_own)
    for c in to_partner:
        c.wait()
    a_own[...] += z_recv_a[...]
    y_own[...] += z_recv_y[...]

    def a_copy(o):
        return y_copy(1, o, a_own, a_own)

    def l_copy(o):
        return y_copy(2, o, y_own, y_own)

    run(ny, a_copy, "start")
    run(ny, l_copy, "start")

    run(ny, p1_copy, "wait")
    for t in range(nx):
        target = (t * ny + iy) * nz + iz
        there = dev == target
        for i in range(IFACES):
            low_need = there & (box == i)
            high_need = there & (box == i - 1)
            code = jnp.where(low_need, far_dev[0], jnp.where(high_need, far_dev[1], -1))
            source = jnp.maximum(jnp.max(code), 0)
            sy = lax.rem(lax.div(source, nz), ny)
            at = SLOTS if i == 0 else (0 if i == SLOTS else i)
            p2_send[t, 3 * i : 3 * i + 3] = p1_buf[sy, 3 * at : 3 * at + 3]
        p2_send[t, PLANE_ROWS - 1 : PLANE_ROWS] = jnp.zeros((1, F * F), jnp.float32)
    p2_buf[ix] = p2_send[ix]

    def p2_copy(o):
        return x_copy(0, o, p2_send.at[x_peer(o)], p2_buf.at[ix])

    run(nx, p2_copy, "start")

    visc_load.wait()
    slots = []
    for s in range(SLOTS):
        here = slot == me * SLOTS + s
        b = pick(here, box)
        near = []
        for side in range(2):
            m = pick(here, near_slot[side])
            n = jnp.maximum(m, 0)
            d = lax.div(n, SLOTS)
            near.append((m >= 0, d == me, lax.rem(n, SLOTS), lax.div(d, ny * nz)))
        slots.append((b >= 0, jnp.maximum(b, 0), near))
    homes = [pick(dev == (t * ny + iy) * nz + iz, home) for t in range(nx)]
    holders = [
        [jnp.maximum(pick((brick == (ix * ny + t) * nz + iz) & (box == j), slot), 0) for j in range(SLOTS)]
        for t in range(ny)
    ]

    lane = lax.broadcasted_iota(jnp.int32, (F, F * F), 1)
    row = lax.broadcasted_iota(jnp.int32, (F, F * F), 0)
    lz = lane % F

    def bulk(s, c):
        cv = step_rate * visc[s]
        for k in range(3):
            v = fine[k, s]
            total = jnp.where(row == 0, 0.0, pltpu.roll(v, 1, 0))
            total += jnp.where(row == F - 1, 0.0, pltpu.roll(v, F - 1, 0))
            total += jnp.where(lane < F, 0.0, pltpu.roll(v, F, 1))
            total += jnp.where(lane >= F * F - F, 0.0, pltpu.roll(v, F * F - F, 1))
            total += jnp.where(lz == 0, 0.0, pltpu.roll(v, 1, 1))
            total += jnp.where(lz == F - 1, 0.0, pltpu.roll(v, F * F - 1, 1))
            at = pl.multiple_of((s * 3 + k) * F, F)
            value = v + cv * (total - 6.0 * v)
            advs[0, pl.ds(at, F)] = value[:, :LANES]
            advs[1, pl.ds(at, F)] = value[:, LANES:]
        return c

    lax.fori_loop(0, SLOTS, bulk, 0)

    run(ny, a_copy, "wait")
    run(ny, l_copy, "wait")
    lines_load.wait()
    half = bx // 2
    low_line = rem(line_id, 2) == 0
    for t in range(nx):
        code = jnp.maximum(homes[t], 0)
        hx, hy = lax.div(code, ny), lax.rem(code, ny)
        d = hx - ix
        same, up_one, down_one = as_float(d == 0), as_float(d == 1), as_float(d == -1)
        lower = y_buf[jnp.maximum(hy - 1, 0)] * as_float(hy > 0)
        upper = y_buf[jnp.minimum(hy + 1, ny - 1)] * as_float(hy < ny - 1)
        extra = exact_right(jnp.where(low_line, lower, upper), lines[...])
        own = a_buf[hy]
        e_send[t, 0:half] = (own[0:half] + extra[0:half, 0:LANES]) * same
        e_send[t, half:bx] = (own[half:bx] + extra[0:half, LANES : 2 * LANES]) * same
        e_send[t, bx : bx + 1] = (own[bx : bx + 1] + extra[half : half + 1, 0:LANES]) * up_one
        e_send[t, bx + 1 : bx + 2] = (own[bx + 1 : bx + 2] + extra[half + 1 : half + 2, 0:LANES]) * down_one
        for k in range(3):
            for side in range(2):
                at = bx + 2 + 2 * k + side
                first = (2 + 2 * k + side) * LANES
                from_row = 0 if side == 0 else half - 1
                inner = own[at : at + 1] + extra[from_row : from_row + 1, first : first + LANES]
                first = (2 + 2 * k) * LANES
                outer = own[at + 6 : at + 7] + extra[half + side : half + side + 1, first : first + LANES]
                e_send[t, at : at + 1] = inner * (0.25 * same) + outer * (0.75 * (down_one if side else up_one))
    e_buf[ix] = e_send[ix]

    def e_copy(o):
        return x_copy(1, o, e_send.at[x_peer(o)], e_buf.at[ix])

    run(nx, e_copy, "start")

    shape = (SLOTS * F, E_ROWS)
    out_line = lax.broadcasted_iota(jnp.int32, shape, 0)
    from_line = lax.broadcasted_iota(jnp.int32, shape, 1)
    boxes = jnp.full(shape, slots[0][1], jnp.int32)
    for s in range(1, SLOTS):
        boxes = jnp.where(out_line // F == s, slots[s][1], boxes)
    f_id = out_line % F
    center = B * boxes + f_id // 2
    other = jnp.where(f_id % 2 == 0, center - 1, center + 1)
    other = jnp.where(other < 0, bx, jnp.where(other >= bx, bx + 1, other))
    blend = jnp.where(from_line == center, 0.75, jnp.where(from_line == other, 0.25, 0.0))
    run(nx, p2_copy, "wait")
    ghost_load.wait()
    run(nx, e_copy, "wait")
    total = e_buf[0]
    for t in range(1, nx):
        total += e_buf[t]
    along = exact_left(blend, total)
    ghosts = exact_right(along, ghost[:, 0 : 3 * F * F])
    faces = exact_right(total[bx : E_ROWS], ghost[:, 3 * F * F :])
    mean_load.wait()
    for s in range(SLOTS):
        active, b, near = slots[s]
        cv = step_rate * visc[s]
        for k in range(3):
            ends = []
            for side in range(2):
                has, is_local, n, sx = near[side]
                x = (F - 1) * (1 - side)
                far = p2_buf[sx, pl.ds(3 * (b + side) + k, 1)]
                here = fine[k, n][x : x + 1]
                outer = faces[2 + 2 * k + side : 3 + 2 * k + side]
                ends.append(jnp.where(has, jnp.where(is_local, here, far), outer))
            edge = jnp.where(row == 0, ends[0], jnp.where(row == F - 1, ends[1], 0.0))
            at = (s * 3 + k) * F
            ghost_k = ghosts[s * F : s * F + F, k * F * F : (k + 1) * F * F]
            adv = jnp.concatenate([advs[0, at : at + F], advs[1, at : at + F]], axis=1) + cv * (ghost_k + edge)
            advs[0, at : at + F] = adv[:, :LANES]
            advs[1, at : at + F] = adv[:, LANES:]
            fine_out[k, s] = jnp.where(active, adv, 0.0)
    rows = 3 * SLOTS * F // 2
    pairs = [advs[h, pl.ds(0, rows, 2)] + advs[h, pl.ds(1, rows, 2)] for h in range(2)]
    z = exact_right(jnp.concatenate(pairs, axis=1), mean[...])
    lane_m = lax.broadcasted_iota(jnp.int32, (B // 2, LANES), 1)
    for s in range(SLOTS):
        for k in range(3):
            at = (s * 3 + k) * B
            value = jnp.where(lane_m < 64, z[at : at + B // 2], z[at + B // 2 : at + B])
            m_send[s, k * (B // 2) : (k + 1) * (B // 2)] = value

    def m_copy(o):
        return x_copy(2, o, m_send, m_buf.at[ix])

    run(nx, m_copy, "start")
    m_buf[ix] = m_send[...]
    run(nx, m_copy, "wait")
    for t in range(ny):
        for j in range(SLOTS):
            n = holders[t][j]
            q_send[t, j] = m_buf[lax.div(n, SLOTS * nz * ny), lax.rem(n, SLOTS)]

    def q_copy(o):
        return y_copy(3, o, q_send.at[y_peer(o)], q_buf.at[iy])

    run(ny, q_copy, "start")
    q_buf[iy] = q_send[iy]
    owners = [
        jnp.maximum(pick((brick == me) & (box == j), slot), 0) for j in range(SLOTS)
    ]
    run(ny, q_copy, "wait")
    for j in range(SLOTS):
        picked[j] = q_buf[lax.rem(lax.div(owners[j], SLOTS * nz), ny), j]


def final_kernel(dims, corners, slot_ref, field, picked, fine, coarse_out, fine_out, group, sems):
    nx, ny, nz, bx, by, bz = dims
    ix, iy, iz = lax.axis_index("gx"), lax.axis_index("gy"), lax.axis_index("gz")
    me = (ix * ny + iy) * nz + iz
    _, _, _, brick, place = grid_tables((bx, by, bz), ny, nz, corners, slot_ref)
    code = pick(brick == me, place)
    present = code >= 0
    code = jnp.maximum(code, 0)
    y_group = lax.div(lax.div(code, bz), B)
    z = lax.rem(code, bz)
    fine_copy = pltpu.make_async_copy(fine, fine_out, sems.at[0])
    fine_copy.start()

    def plain(g):
        return pltpu.make_async_copy(
            field.at[:, pl.ds(g * B, B)], coarse_out.at[:, pl.ds(g * B, B)], sems.at[1 + g]
        )

    def patched(g):
        return pltpu.make_async_copy(group, coarse_out.at[:, pl.ds(g * B, B)], sems.at[1 + g])

    for g in range(by // B):

        @pl.when(y_group != g)
        def _():
            plain(g).start()

    start = pl.multiple_of(y_group * B, B)
    low = lax.rem(z, LANES)
    tile = lax.div(z, LANES)
    lane = lax.broadcasted_iota(jnp.int32, (B, LANES), 1)
    eight = lane // B
    line = lax.broadcasted_iota(jnp.int32, (B, LANES), 0)
    chosen = eight % B == line
    first_half = (eight - line + 16) % 16 < B
    inside = [(lane >= low) & (lane < low + B) & (tile == t) & present for t in range(bz // LANES)]
    for j in range(SLOTS):
        for at in range(MEAN_ROWS):
            value = jnp.where(chosen, jnp.broadcast_to(picked[j, at : at + 1], (B, LANES)), 0.0)
            for step in (B, 2 * B, 4 * B):
                value += pltpu.roll(value, step, 1)
            swapped = pltpu.roll(value, 64, 1)
            k, a = at // (B // 2), at % (B // 2)
            for h in range(2):
                new = jnp.where(first_half, value, swapped) if h == 0 else jnp.where(first_half, swapped, value)
                x = k * bx + j * B + h * (B // 2) + a
                for t in range(bz // LANES):
                    old = field[x, pl.ds(start, B), t * LANES : (t + 1) * LANES]
                    group[x, :, t * LANES : (t + 1) * LANES] = jnp.where(inside[t], new, old)
    patched(y_group).start()
    for g in range(by // B):
        patched(g).wait()
    fine_copy.wait()


def on_device(coarse_field, fine_field, viscosity, corners, grid_slot, neighbors):
    nx, ny, nz = (lax.axis_size(n) for n in ("gx", "gy", "gz"))
    assert nz == 2
    bx, by, bz = coarse_field.shape[1:]
    dims = (nx, ny, nz, bx, by, bz)
    consts = matrices()
    vmem = pl.BlockSpec(memory_space=pltpu.VMEM)
    hbm = pl.BlockSpec(memory_space=pltpu.HBM)
    stay = functools.partial(pltpu.with_memory_space_constraint, memory_space=pltpu.HBM)
    grids = grid_slot.shape[0]
    f32 = jnp.float32
    dma = pltpu.SemaphoreType.DMA
    tables_in = (corners.T, grid_slot.reshape(1, -1))
    fine_new, picked = pl.pallas_call(
        functools.partial(step_kernel, dims),
        out_shape=(
            jax.ShapeDtypeStruct(fine_field.shape, f32),
            jax.ShapeDtypeStruct((SLOTS, MEAN_ROWS, LANES), f32),
        ),
        in_specs=[hbm] * 10,
        out_specs=(vmem, vmem),
        scratch_shapes=[
            pltpu.VMEM((3, grids), jnp.int32),
            pltpu.VMEM((1, grids), jnp.int32),
            pltpu.VMEM((2, grids), jnp.int32),
            pltpu.VMEM((bz // LANES, 3 * bx * by, LANES), f32),
            pltpu.VMEM(fine_field.shape, f32),
            pltpu.VMEM(viscosity.shape, f32),
        ]
        + [pltpu.VMEM(c.shape, c.dtype) for c in consts]
        + [
            pltpu.VMEM((3, E_ROWS, LANES), f32),
            pltpu.VMEM((A_ROWS, LANES), f32),
            pltpu.VMEM((Y_ROWS, LANES), f32),
            pltpu.VMEM((A_ROWS, LANES), f32),
            pltpu.VMEM((Y_ROWS, LANES), f32),
            pltpu.VMEM((ny, A_ROWS, LANES), f32),
            pltpu.VMEM((ny, Y_ROWS, LANES), f32),
            pltpu.VMEM((ny, PLANE_ROWS, F * F), f32),
            pltpu.VMEM((nx, PLANE_ROWS, F * F), f32),
            pltpu.VMEM((nx, PLANE_ROWS, F * F), f32),
            pltpu.VMEM((nx, E_ROWS, LANES), f32),
            pltpu.VMEM((nx, E_ROWS, LANES), f32),
            pltpu.VMEM((2, 3 * SLOTS * F, LANES), f32),
            pltpu.VMEM((SLOTS, MEAN_ROWS, LANES), f32),
            pltpu.VMEM((nx, SLOTS, MEAN_ROWS, LANES), f32),
            pltpu.VMEM((ny, SLOTS, MEAN_ROWS, LANES), f32),
            pltpu.VMEM((ny, SLOTS, MEAN_ROWS, LANES), f32),
            dma((9 + bz // LANES,)),
            dma((2, 2)),
            dma((4, ny)),
            dma((4, ny)),
            dma((3, nx)),
            dma((3, nx)),
        ],
        compiler_params=pltpu.CompilerParams(collective_id=0, has_side_effects=True, vmem_limit_bytes=24 * MIB),
        name="step",
    )(
        *map(
            stay, (*tables_in, neighbors.T, coarse_field.reshape(3 * bx * by, bz), fine_field, viscosity, *consts)
        )
    )
    coarse_out, fine_out = pl.pallas_call(
        functools.partial(final_kernel, dims),
        out_shape=(
            jax.ShapeDtypeStruct((3 * bx, by, bz), f32),
            jax.ShapeDtypeStruct(fine_field.shape, f32),
        ),
        in_specs=[vmem] * 5,
        out_specs=(hbm, hbm),
        scratch_shapes=[pltpu.VMEM((3 * bx, B, bz), f32), dma((1 + by // B,))],
        compiler_params=pltpu.CompilerParams(vmem_limit_bytes=16 * MIB),
        name="final",
    )(*tables_in, coarse_field.reshape(3 * bx, by, bz), picked, fine_new)
    return fine_out, coarse_out.reshape(coarse_field.shape)


def solution(mesh):
    in_specs = (
        P(None, "gx", "gy", "gz"),
        P(None, ("gx", "gy", "gz"), None, None),
        P(("gx", "gy", "gz"), None, None),
        P(),
        P(),
        P(),
    )
    out_specs = (P(None, ("gx", "gy", "gz"), None, None), P(None, "gx", "gy", "gz"))
    return jax.shard_map(
        on_device, mesh=mesh, in_specs=in_specs, out_specs=out_specs, check_vma=False
    )
```

```python
import functools
import numpy as np
import jax
import jax.numpy as jnp
from jax import lax
from jax.experimental import pallas as pl
from jax.experimental.pallas import tpu as pltpu
from jax.sharding import PartitionSpec as P

B = 8
F = 16
SLOTS = 4
SIDE = B + 2
LANES = 128
WIDE = 4 * SIDE
IFACES = SLOTS + 1
PLANE_LINES = 4
E_ROWS = 48
MEAN_ROWS = 12
step_rate = 0.15
MIB = 1 << 20


def tables():
    tangent = np.zeros((F, SIDE), np.float32)
    for f in range(F):
        c = f // 2 + 1
        tangent[f, c] = 0.75
        tangent[f, c - 1 if f % 2 == 0 else c + 1] = 0.25
    low = np.zeros((SIDE,), np.float32)
    low[0], low[1] = 0.75, 0.25
    return tangent, low, low[::-1].copy()


def matrices():
    tangent, low, high = tables()
    eye = np.eye(SIDE, dtype=np.float32)
    cut = np.zeros((SIDE, SIDE, 4, SIDE), np.float32)
    cut[:, :, 0] = np.einsum("b,cd->bcd", low, eye)
    cut[:, :, 1] = np.einsum("b,cd->bcd", high, eye)
    cut[:, :, 2] = np.einsum("bd,c->bcd", eye, low)
    cut[:, :, 3] = np.einsum("bd,c->bcd", eye, high)
    put = np.zeros((4, SIDE, F, F), np.float32)
    put[0, :, 0, :] = tangent.T
    put[1, :, F - 1, :] = tangent.T
    put[2, :, :, 0] = tangent.T
    put[3, :, :, F - 1] = tangent.T
    columns = np.zeros((3, LANES, LANES), np.float32)
    lines = np.zeros((LANES, 8, LANES), np.float32)
    ghost = np.zeros((LANES, 4, F * F), np.float32)
    for k in range(3):
        columns[k, : SIDE * SIDE, k * WIDE : (k + 1) * WIDE] = cut.reshape(SIDE * SIDE, WIDE)
        ghost[k * WIDE : (k + 1) * WIDE, k] = put.reshape(WIDE, F * F)
        for half in range(2):
            for side in range(2):
                for c in range(SIDE):
                    lane = half * 64 + k * 2 * SIDE + side * SIDE + c
                    window = side * (SIDE - 1) * SIDE + c
                    lines[lane, half] = columns[k, window]
                    lines[lane, 2 + 2 * k + half, window] = 1.0
    ghost[: SIDE * SIDE, 3] = np.einsum("sb,tc->bcst", tangent, tangent).reshape(SIDE * SIDE, F * F)
    mean = np.zeros((F * F, LANES), np.float32)
    for y in range(F):
        for z in range(F):
            for half in range(2):
                mean[y * F + z, half * 64 + (y // 2) * B + z // 2] = 0.125
    rim = [y * F + z for y in range(F) for z in range(F) if y in (0, F - 1) or z in (0, F - 1)]
    take = np.zeros((F * F, LANES), np.float32)
    rim_ghost = np.zeros((LANES, 3, LANES), np.float32)
    rim_mean = np.zeros((LANES, LANES), np.float32)
    for m, at in enumerate(rim):
        for half in range(2):
            take[at, half * 64 + m] = 1.0
            rim_ghost[:, :, half * 64 + m] = ghost[:, :3, at]
            rim_mean[half * 64 + m, half * 64 + (at // F // 2) * B + at % F // 2] = 0.125
    shapes = (
        columns.reshape(3 * LANES, LANES), lines.reshape(LANES, 8 * LANES), ghost.reshape(LANES, 4 * F * F),
        mean, take, rim_ghost.reshape(LANES, 3 * LANES), rim_mean,
    )
    return tuple(jnp.asarray(a, jnp.bfloat16) for a in shapes)


def div(a, n):
    return lax.div(a, jnp.full_like(a, n))


def rem(a, n):
    return lax.rem(a, jnp.full_like(a, n))


def split(a):
    high = a.astype(jnp.bfloat16)
    return high, (a - high.astype(jnp.float32)).astype(jnp.bfloat16)


def dot(a, b):
    return jnp.dot(a, b, preferred_element_type=jnp.float32)


def exact_right(a, b):
    high, low = split(a)
    return dot(high, b) + dot(low, b)


def exact_left(a, b):
    a = a.astype(jnp.bfloat16)
    high, low = split(b)
    return dot(a, high) + dot(a, low)


def pick(mask, value):
    return jnp.max(jnp.where(mask, value, -1))


def as_float(cond):
    return jnp.where(cond, 1.0, 0.0).astype(jnp.float32)


def grid_tables(bricks, ny, nz, corners, slot_ref):
    x, y, z = corners[0:1, :], corners[1:2, :], corners[2:3, :]
    slot = slot_ref[...]
    brick = (div(x, bricks[0]) * ny + div(y, bricks[1])) * nz + div(z, bricks[2])
    place = rem(y, bricks[1]) * bricks[2] + rem(z, bricks[2])
    return x, y, slot, brick, place


def step_kernel(
    dims, corners_in, slot_in, near_in, coarse, fine_in, visc_in,
    columns_in, lines_in, ghost_in, mean_in, take_in, rim_ghost_in, rim_mean_in,
    fine_out, picked,
    corners, slot_ref, near_ref, field, fine, visc, columns, lines, ghost, mean, take, rim_ghost, rim_mean,
    window, z_send, z_recv, w_buf, p_buf, f_buf, p2_send, p2_buf, e_send, e_buf,
    advs, m_send, m_buf, c_send, c_buf, qm_send, qm_buf, qc_send, qc_buf, qf_send, qf_buf,
    local_sem, z_sem, y_send_sem, y_recv_sem, x_send_sem, x_recv_sem,
):
    nx, ny, nz, bx, by, bz = dims
    ix, iy, iz = lax.axis_index("gx"), lax.axis_index("gy"), lax.axis_index("gz")
    me = (ix * ny + iy) * nz + iz
    mesh_id = pl.DeviceIdType.MESH
    tiles = bz // LANES
    half = bx // 2
    pitch = by + 8

    pairs = [
        (corners_in, corners), (slot_in, slot_ref), (near_in, near_ref), (fine_in, fine), (visc_in, visc),
    ]
    for t in range(tiles):
        pairs.append((coarse.at[:, :, t * LANES : (t + 1) * LANES], field.at[t, :, 0:by]))
    pairs += [
        (mean_in, mean), (take_in, take), (columns_in, columns), (lines_in, lines), (ghost_in, ghost),
        (rim_ghost_in, rim_ghost), (rim_mean_in, rim_mean),
    ]
    loads = [pltpu.make_async_copy(src, dst, local_sem.at[i]) for i, (src, dst) in enumerate(pairs)]
    for load in loads:
        load.start()
    table_loads, fine_load, visc_load, field_loads = loads[:3], loads[3], loads[4], loads[5 : 5 + tiles]
    mean_load, take_load, columns_load, lines_load, ghost_load, rim_ghost_load, rim_mean_load = loads[5 + tiles :]

    def y_peer(o):
        return lax.rem(iy + o, ny)

    def x_peer(o):
        return lax.rem(ix + o, nx)

    barrier = pltpu.get_barrier_semaphore()
    pl.semaphore_signal(barrier, inc=1, device_id={"gz": 1 - iz}, device_id_type=mesh_id)

    def greet_y(o, c):
        pl.semaphore_signal(barrier, inc=1, device_id={"gy": y_peer(o)}, device_id_type=mesh_id)
        return c

    def greet_x(o, c):
        pl.semaphore_signal(barrier, inc=1, device_id={"gx": x_peer(o)}, device_id_type=mesh_id)
        return c

    lax.fori_loop(1, ny, greet_y, 0)
    lax.fori_loop(1, nx, greet_x, 0)

    def y_copy(which, o, src, dst):
        return pltpu.make_async_remote_copy(
            src_ref=src, dst_ref=dst, send_sem=y_send_sem.at[which, o - 1], recv_sem=y_recv_sem.at[which, o - 1],
            device_id={"gy": y_peer(o)}, device_id_type=mesh_id,
        )

    def x_copy(which, o, src, dst):
        return pltpu.make_async_remote_copy(
            src_ref=src, dst_ref=dst, send_sem=x_send_sem.at[which, o - 1], recv_sem=x_recv_sem.at[which, o - 1],
            device_id={"gx": x_peer(o)}, device_id_type=mesh_id,
        )

    def run(count, makes, action):
        def body(o, c):
            for make in makes:
                getattr(make(o), action)()
            return c

        lax.fori_loop(1, count, body, 0)

    for load in table_loads:
        load.wait()
    gx_, gy_, slot, brick, place = grid_tables((bx, by, bz), ny, nz, corners, slot_ref)
    home = div(gx_, bx) * ny + div(gy_, by)
    box = div(rem(gx_, bx), B)
    dev = div(slot, SLOTS)
    count = slot.shape[1]
    g_row = lax.broadcasted_iota(jnp.int32, (count, count), 0)
    g_col = lax.broadcasted_iota(jnp.int32, (count, count), 1)
    slot_col = jnp.max(jnp.where(g_row == g_col, slot, -1), axis=1, keepdims=True)
    near_slot = []
    far_dev = []
    for side in range(2):
        m = jnp.max(jnp.where(g_row == near_ref[side : side + 1, :], slot_col, -1), axis=0, keepdims=True)
        near_slot.append(m)
        d = div(jnp.maximum(m, 0), SLOTS)
        far_dev.append(jnp.where((m >= 0) & (d != dev), d, -1))

    def anchor(ox, oy, gz):
        hx, hy = ix + ox, iy + oy
        inside = (hx >= 0) & (hx < nx) & (hy >= 0) & (hy < ny)
        code = jnp.maximum(pick(brick == jnp.where(inside, (hx * ny + hy) * nz + gz, -5), place), 0)
        return lax.div(code, bz), lax.rem(code, bz)

    mine = dev == me
    own_slot = [pick(mine & (box == j), rem(slot, SLOTS)) for j in range(SLOTS)]
    slots = []
    for s in range(SLOTS):
        here = slot == me * SLOTS + s
        b = pick(here, box)
        near = []
        for side in range(2):
            m = pick(here, near_slot[side])
            n = jnp.maximum(m, 0)
            d = lax.div(n, SLOTS)
            near.append((m >= 0, d == me, lax.rem(n, SLOTS), lax.div(d, ny * nz)))
        slots.append((b >= 0, jnp.maximum(b, 0), near))
    anchors = [
        {(ox, oy): anchor(ox, oy, gz) for ox in (-1, 0, 1) for oy in (-1, 0, 1)} for gz in (1 - iz, iz)
    ]

    fine_load.wait()
    visc_load.wait()
    for i in range(IFACES):
        below = jnp.maximum(own_slot[max(i - 1, 0)], 0)
        above = jnp.maximum(own_slot[min(i, SLOTS - 1)], 0)
        for k in range(PLANE_LINES):
            def line(n, x):
                return fine[k, n, x : x + 1] if k < 3 else step_rate * visc[n, x : x + 1]

            if i == 0:
                value = line(above, 0)
            elif i == SLOTS:
                value = line(below, F - 1)
            else:
                value = jnp.where(own_slot[i - 1] >= 0, line(below, F - 1), line(above, 0))
            p_buf[iy, i, k : k + 1] = value
    pl.semaphore_wait(barrier, nx + ny - 1)
    own_planes = p_buf.at[iy]

    def p1_copy(o):
        return y_copy(0, o, own_planes, own_planes)

    def f_copy(o):
        return x_copy(0, o, own_planes, f_buf.at[ix])

    run(ny, [p1_copy], "start")
    run(nx, [f_copy], "start")
    f_buf[ix] = p_buf[iy]

    lane = lax.broadcasted_iota(jnp.int32, (F, F * F), 1)
    row = lax.broadcasted_iota(jnp.int32, (F, F * F), 0)
    lz = lane % F
    for s in range(SLOTS):
        cv = step_rate * visc[s]
        for k in range(3):
            v = fine[k, s]
            ends = []
            for side in range(2):
                has, is_local, n, _ = slots[s][2][side]
                x = (F - 1) * (1 - side)
                ends.append(fine[k, n][x : x + 1] * as_float(has & is_local))
            total = jnp.where(row == 0, ends[0], pltpu.roll(v, 1, 0))
            total += jnp.where(row == F - 1, ends[1], pltpu.roll(v, F - 1, 0))
            total += jnp.where(lane < F, 0.0, pltpu.roll(v, F, 1))
            total += jnp.where(lane >= F * F - F, 0.0, pltpu.roll(v, F * F - F, 1))
            total += jnp.where(lz == 0, 0.0, pltpu.roll(v, 1, 1))
            total += jnp.where(lz == F - 1, 0.0, pltpu.roll(v, F * F - 1, 1))
            at = (s * 3 + k) * F
            value = v + cv * (total - 6.0 * v)
            advs[0, at : at + F] = value[:, :LANES]
            advs[1, at : at + F] = value[:, LANES:]
    rows = 3 * SLOTS * F // 2
    mean_load.wait()
    sums = [advs[h, pl.ds(0, rows, 2)] + advs[h, pl.ds(1, rows, 2)] for h in range(2)]
    z = exact_right(jnp.concatenate(sums, axis=1), mean[...])
    quarter = B // 2
    lane_m = lax.broadcasted_iota(jnp.int32, (quarter, LANES), 1)
    for s in range(SLOTS):
        for k in range(3):
            at = (s * 3 + k) * B
            m_send[s, k * quarter : (k + 1) * quarter] = jnp.where(
                lane_m < 64, z[at : at + quarter], z[at + quarter : at + B]
            )
    take_load.wait()
    lane_f = lax.broadcasted_iota(jnp.int32, (F, LANES), 1)
    rims = exact_right(step_rate * visc[...].reshape(SLOTS * F, F * F), take[...])
    for s in range(SLOTS // 2):
        low, high = rims[s * F : (s + 1) * F], rims[(s + 2) * F : (s + 3) * F]
        c_send[s] = jnp.where(lane_f < 64, low, high)

    def m_copy(o):
        return x_copy(1, o, m_send, m_buf.at[ix])

    def c_copy(o):
        return x_copy(2, o, c_send, c_buf.at[ix])

    run(nx, [m_copy, c_copy], "start")
    m_buf[ix] = m_send[...]
    c_buf[ix] = c_send[...]

    flat = field.reshape(tiles, 3 * bx * pitch, LANES)
    stride = bx * pitch
    lane1 = lax.broadcasted_iota(jnp.int32, (1, LANES), 1)
    lane_b = div(lane1, SIDE)
    lane_c = rem(lane1, SIDE)
    half_lane = rem(lane1, 64)
    half_c = rem(half_lane, SIDE)
    line_id = div(half_lane, SIDE)

    def shifted(z, same, start, size, step, to):
        def get(t):
            return flat[t, pl.ds(start, size, step)] if size > 1 else flat[t, pl.ds(start, 1)]

        z = lax.rem(z - 1 + bz, bz)
        tile, low = lax.div(z, LANES), lax.rem(z, LANES)
        if same:
            lane = lax.broadcasted_iota(jnp.int32, (size, LANES), 1)
            value = jnp.where(lane >= low, get(tile), get(lax.rem(tile + 1, tiles)))
        else:
            value = get((tiles - 1) * (1 - iz))
        return pltpu.roll(value, lax.rem(to - low + LANES, LANES), 1)

    def z_weight(z, ids, same):
        first, last = z == 0, z == bz - B
        if same:
            return jnp.where(ids == 0, as_float(~first), jnp.where(ids == SIDE - 1, as_float(~last), 1.0))
        first = as_float(first & (iz == 0))
        last = as_float(last & (iz == 1))
        return jnp.where(ids == 0, first, jnp.where(ids == SIDE - 1, last, 0.0))

    def weights(y, z, same):
        weight = z_weight(z, lane_c, same)
        weight = weight * jnp.where(
            lane_b == 0, as_float(y > 0), jnp.where(lane_b == SIDE - 1, as_float(y < by - B), 1.0)
        )
        return jnp.where(lane1 < SIDE * SIDE, weight, 0.0)

    edge_at = bx + half
    line_at = edge_at + 2
    inner_at = line_at + 2
    outer_at = inner_at + 6

    def pack(place, same, to_ref):
        y, z = place[0, 0]
        weight = weights(y, z, same)
        for k in range(3):
            acc = jnp.zeros((bx, LANES), jnp.float32)
            for b in range(SIDE):
                at = jnp.clip(y - 1 + b, 0, by - 1)
                value = shifted(z, same, k * stride + at, bx, pitch, SIDE * b)
                acc = jnp.where(lane_b == b, value, acc)
            window[k, 0:bx] = acc * weight
        for n, ox in enumerate((1, -1)):
            y, z = place[ox, 0]
            weight = weights(y, z, same)
            x = bx - 1 if ox > 0 else 0
            acc = jnp.zeros((3, LANES), jnp.float32)
            for b in range(SIDE):
                at = jnp.clip(y - 1 + b, 0, by - 1)
                acc = jnp.where(lane_b == b, shifted(z, same, x * pitch + at, 3, stride, SIDE * b), acc)
            acc = acc * weight
            for k in range(3):
                window[k, bx + n : bx + n + 1] = acc[k : k + 1]
        total = jnp.zeros((bx + 8, LANES), jnp.float32)
        for k in range(3):
            total += exact_right(window[k], columns[k * LANES : (k + 1) * LANES])
            for side in range(2):
                at = inner_at + 2 * k + side
                inner = 0 if side == 0 else bx - 1
                to_ref[at : at + 1] = window[k, inner : inner + 1]
                to_ref[at + 6 : at + 7] = window[k, bx + side : bx + side + 1]
        to_ref[0:bx] = total[0:bx]
        to_ref[edge_at : edge_at + 2] = total[bx : bx + 2]
        main = [jnp.zeros((half, LANES), jnp.float32) for _ in range(2)]
        ends = [jnp.zeros((1, LANES), jnp.float32) for _ in range(2)]
        for side, oy in enumerate((1, -1)):
            at = by - 1 if oy > 0 else 0
            edge = 0 if oy > 0 else by - B
            y, z = place[0, oy]
            weight = z_weight(z, half_c, same) * as_float(y == edge)
            for k in range(3):
                to = k * 2 * SIDE + side * SIDE
                for h in range(2):
                    value = shifted(z, same, k * stride + h * half * pitch + at, half, pitch, to + 64 * h)
                    main[h] = jnp.where(line_id == 2 * k + side, value * weight, main[h])
            for n, ox in enumerate((1, -1)):
                y, z = place[ox, oy]
                weight = z_weight(z, half_c, same) * as_float(y == edge)
                x = bx - 1 if ox > 0 else 0
                for k in range(3):
                    to = k * 2 * SIDE + side * SIDE
                    value = shifted(z, same, k * stride + x * pitch + at, 1, 1, to)
                    ends[n] = jnp.where(line_id == 2 * k + side, value * weight, ends[n])
        to_ref[bx:edge_at] = jnp.where(lane1 < 64, main[0], main[1])
        for n in range(2):
            to_ref[line_at + n : line_at + n + 1] = jnp.where(lane1 < 64, ends[n], 0.0)

    own = w_buf.at[iy]
    for k in range(3):
        window[k, bx + 2 : bx + 8] = jnp.zeros((6, LANES), jnp.float32)
    for load in field_loads:
        load.wait()
    columns_load.wait()
    pack(anchors[0], False, z_send)
    z_copy = pltpu.make_async_remote_copy(
        src_ref=z_send, dst_ref=z_recv, send_sem=z_sem.at[0], recv_sem=z_sem.at[1],
        device_id={"gz": 1 - iz}, device_id_type=mesh_id,
    )
    z_copy.start()
    pack(anchors[1], True, own)
    z_copy.wait()
    own[...] += z_recv[...]

    def w_copy(o):
        return y_copy(1, o, own, own)

    run(ny, [w_copy], "start")

    run(ny, [p1_copy], "wait")
    for t in range(nx):
        there = dev == (t * ny + iy) * nz + iz
        for i in range(IFACES):
            code = jnp.where(there & (box == i), far_dev[0], jnp.where(there & (box == i - 1), far_dev[1], -1))
            sy = lax.rem(lax.div(jnp.maximum(jnp.max(code), 0), nz), ny)
            at = SLOTS if i == 0 else (0 if i == SLOTS else i)
            p2_send[t, i] = p_buf[sy, at]
    p2_buf[ix] = p2_send[ix]

    def p2_copy(o):
        return x_copy(3, o, p2_send.at[x_peer(o)], p2_buf.at[ix])

    run(nx, [p2_copy], "start")

    homes = [pick(dev == (t * ny + iy) * nz + iz, home) for t in range(nx)]

    def brick_plan(t):
        here = brick == (ix * ny + t) * nz + iz
        held = [pick(here & (box == j), slot) for j in range(SLOTS)]
        low = pick(here & (box == 0), near_slot[0])
        high = pick(here & (box == SLOTS - 1), near_slot[1])
        near = [(held[j - 1] if j > 0 else low, held[j + 1] if j < SLOTS - 1 else high) for j in range(SLOTS)]
        return [jnp.maximum(n, 0) for n in held], near

    bricks = [brick_plan(t) for t in range(ny)]
    own_held, own_near = brick_plan(iy)

    run(ny, [w_copy], "wait")
    lines_load.wait()
    low_line = rem(line_id, 2) == 0
    target_home = [jnp.maximum(h, 0) for h in homes]
    target_x = [lax.div(h, ny) for h in target_home] + [ix]
    target_y = [lax.rem(h, ny) for h in target_home] + [iy]
    mixed = []
    for hy in target_y:
        before, after = jnp.maximum(hy - 1, 0), jnp.minimum(hy + 1, ny - 1)
        low_on, high_on = as_float(hy > 0), as_float(hy < ny - 1)
        for first, last in ((bx, edge_at), (line_at, line_at + 2)):
            low, high = w_buf[before, first:last] * low_on, w_buf[after, first:last] * high_on
            mixed.append(jnp.where(low_line, low, high))
        mixed.append(jnp.zeros((6, LANES), jnp.float32))
    extras = exact_right(jnp.concatenate(mixed, axis=0), lines[...])

    def assemble(n):
        hy = target_y[n]
        extra = extras[n * (half + 8) : (n + 1) * (half + 8)]
        base = w_buf[hy]
        main = (base[0:half] + extra[0:half, 0:LANES], base[half:bx] + extra[0:half, LANES : 2 * LANES])
        ends = base[edge_at : edge_at + 2] + extra[half : half + 2, 0:LANES]
        inner, outer = {}, {}
        for k in range(3):
            for side in range(2):
                at = inner_at + 2 * k + side
                first = (2 + 2 * k + side) * LANES
                from_row = 0 if side == 0 else half - 1
                inner[k, side] = base[at : at + 1] + extra[from_row : from_row + 1, first : first + LANES]
                first = (2 + 2 * k) * LANES
                outer[k, side] = base[at + 6 : at + 7] + extra[half + side : half + side + 1, first : first + LANES]
        return main, ends, inner, outer

    home_main, home_ends, home_inner, home_outer = assemble(nx)
    for t in range(nx):
        main, ends, inner, outer = assemble(t)
        d = target_x[t] - ix
        same, up_one, down_one = as_float(d == 0), as_float(d == 1), as_float(d == -1)
        e_send[t, 0:half] = main[0] * same
        e_send[t, half:bx] = main[1] * same
        e_send[t, bx : bx + 1] = ends[0:1] * up_one
        e_send[t, bx + 1 : bx + 2] = ends[1:2] * down_one
        for k in range(3):
            for side in range(2):
                at = bx + 2 + 2 * k + side
                e_send[t, at : at + 1] = inner[k, side] * (0.25 * same) + outer[k, side] * (
                    0.75 * (down_one if side else up_one)
                )
        above = ix < t
        at = bx + 8
        e_send[t, at : at + 1] = jnp.where(above, home_ends[0:1], home_ends[1:2])
        for k in range(3):
            e_send[t, at + 1 + k : at + 2 + k] = 0.75 * jnp.where(above, home_outer[k, 0], home_outer[k, 1])
        e_send[t, at + 4 : E_ROWS] = jnp.zeros((E_ROWS - at - 4, LANES), jnp.float32)
    e_buf[ix] = e_send[ix]

    def e_copy(o):
        return x_copy(4, o, e_send.at[x_peer(o)], e_buf.at[ix])

    run(nx, [e_copy], "start")

    run(nx, [f_copy, m_copy, c_copy], "wait")
    side_x = SLOTS * nz * ny
    for t in range(ny):
        held, near = bricks[t]
        for j in range(SLOTS):
            n = held[j]
            tx, s = lax.div(n, side_x), lax.rem(n, SLOTS)
            qm_send[t, j] = m_buf[tx, s]
            rim = c_buf[tx, lax.rem(s, 2)]
            flip = lax.div(s, 2) != j // 2
            rim = jnp.where(flip, pltpu.roll(rim, 64, 1), rim)
            keep = lane_f < 64 if j < 2 else lane_f >= 64
            if j < 2:
                qc_send[t, j] = rim
            else:
                qc_send[t, j % 2] = jnp.where(keep, rim, qc_send[t, j % 2])
            for side in range(2):
                other = lax.div(jnp.maximum(near[j][side], 0), side_x)
                if side == 0:
                    at = j if j > 0 else SLOTS
                else:
                    at = j + 1 if j < SLOTS - 1 else 0
                qf_send[t, 2 * j + side, 0:3] = f_buf[other, at, 0:3]
                qf_send[t, 2 * j + side, 3:4] = f_buf[tx, j + side, 3:4]
    qm_buf[iy] = qm_send[iy]
    qc_buf[iy] = qc_send[iy]
    qf_buf[iy] = qf_send[iy]

    def qm_copy(o):
        return y_copy(2, o, qm_send.at[y_peer(o)], qm_buf.at[iy])

    def qc_copy(o):
        return y_copy(3, o, qc_send.at[y_peer(o)], qc_buf.at[iy])

    def qf_copy(o):
        return y_copy(4, o, qf_send.at[y_peer(o)], qf_buf.at[iy])

    run(ny, [qf_copy, qc_copy, qm_copy], "start")

    def blended(boxes_of):
        shape = (SLOTS * F, bx + 8)
        out_line = lax.broadcasted_iota(jnp.int32, shape, 0)
        from_line = lax.broadcasted_iota(jnp.int32, shape, 1)
        boxes = jnp.full(shape, boxes_of[0], jnp.int32)
        for s in range(1, SLOTS):
            boxes = jnp.where(out_line // F == s, boxes_of[s], boxes)
        f_id = out_line % F
        center = B * boxes + f_id // 2
        other = jnp.where(f_id % 2 == 0, center - 1, center + 1)
        other = jnp.where(other < 0, bx, jnp.where(other >= bx, bx + 1, other))
        return jnp.where(from_line == center, 0.75, jnp.where(from_line == other, 0.25, 0.0))

    blend = blended([slots[s][1] for s in range(SLOTS)])
    home_blend = blended(list(range(SLOTS)))
    run(nx, [p2_copy], "wait")
    for load in (ghost_load, rim_ghost_load, rim_mean_load):
        load.wait()
    run(nx, [e_copy], "wait")
    total = e_buf[0, 0 : bx + 8]
    for t in range(1, nx):
        total += e_buf[t, 0 : bx + 8]
    along = exact_left(blend, total)
    ghosts = exact_right(along, ghost[:, 0 : 3 * F * F])
    faces = exact_right(total[bx : bx + 8], ghost[:, 3 * F * F :])
    for s in range(SLOTS):
        active, b, near = slots[s]
        cv = step_rate * visc[s]
        for k in range(3):
            ends = []
            for side in range(2):
                has, is_local, _, sx = near[side]
                far = p2_buf[sx, b + side, k : k + 1]
                outer = faces[2 + 2 * k + side : 3 + 2 * k + side]
                ends.append(jnp.where(has, far * as_float(~is_local), outer))
            edge = jnp.where(row == 0, ends[0], jnp.where(row == F - 1, ends[1], 0.0))
            at = (s * 3 + k) * F
            ghost_k = ghosts[s * F : s * F + F, k * F * F : (k + 1) * F * F]
            adv = jnp.concatenate([advs[0, at : at + F], advs[1, at : at + F]], axis=1) + cv * (ghost_k + edge)
            fine_out[k, s] = jnp.where(active, adv, 0.0)

    before = e_buf[jnp.maximum(ix - 1, 0), bx + 8 : E_ROWS] * as_float(ix > 0)
    after = e_buf[jnp.minimum(ix + 1, nx - 1), bx + 8 : E_ROWS] * as_float(ix < nx - 1)
    face_lines = []
    for k in range(3):
        for side in range(2):
            far = after if side else before
            face_lines.append(0.25 * home_inner[k, side] + far[1 + k : 2 + k])
    home_total = jnp.concatenate([*home_main, before[0:1], after[0:1], *face_lines], axis=0)
    home_along = exact_left(home_blend, home_total)
    rim_ghosts = exact_right(home_along, rim_ghost[...])
    home_faces = exact_right(home_total[bx : bx + 8], ghost[:, 3 * F * F :])
    run(ny, [qf_copy, qc_copy, qm_copy], "wait")

    def row_of(n):
        return lax.rem(lax.div(jnp.maximum(n, 0), SLOTS * nz), ny)

    x_lines = []
    for j in range(SLOTS):
        own_row = row_of(own_held[j])
        own_dev = lax.div(own_held[j], SLOTS)
        for side in range(2):
            m = own_near[j][side]
            other_dev = lax.div(jnp.maximum(m, 0), SLOTS)
            on = as_float((m < 0) | (own_dev != other_dev))
            weight = qf_buf[own_row, 2 * j + side, 3:4] * on
            for k in range(3):
                far = qf_buf[row_of(m), 2 * j + side, k : k + 1]
                x_lines.append(weight * jnp.where(m >= 0, far, home_faces[2 + 2 * k + side : 3 + 2 * k + side]))
    x_means = exact_right(jnp.concatenate(x_lines, axis=0), mean[...])
    products = []
    for j in range(SLOTS // 2):
        low = qc_buf[row_of(own_held[j]), j]
        high = qc_buf[row_of(own_held[j + 2]), j]
        rim = jnp.where(lane_f < 64, low, high)
        for k in range(3):
            low = rim_ghosts[j * F : (j + 1) * F, k * LANES : (k + 1) * LANES]
            high = rim_ghosts[(j + 2) * F : (j + 3) * F, k * LANES : (k + 1) * LANES]
            window[(3 * j + k) // 2, (3 * j + k) % 2 * F : (3 * j + k) % 2 * F + F] = rim * jnp.where(
                lane_f < 64, low, high
            )
    for n in range(3):
        products.append(window[n, pl.ds(0, F, 2)] + window[n, pl.ds(1, F, 2)])
    rim_means = exact_right(jnp.concatenate(products, axis=0), rim_mean[...])
    for j in range(SLOTS):
        own_row = row_of(own_held[j])
        for k in range(3):
            at = (3 * (j % 2) + k) * B
            low, high = rim_means[at : at + quarter], rim_means[at + quarter : at + B]
            if j < 2:
                high = pltpu.roll(high, 64, 1)
            else:
                low = pltpu.roll(low, 64, 1)
            value = qm_buf[own_row, j, k * quarter : (k + 1) * quarter] + jnp.where(lane_m < 64, low, high)
            row_m = lax.broadcasted_iota(jnp.int32, (quarter, LANES), 0)
            for side in range(2):
                n = (2 * j + side) * 3 + k
                place = (row_m == 0) & (lane_m < 64) if side == 0 else (row_m == quarter - 1) & (lane_m >= 64)
                value += jnp.where(place, x_means[n : n + 1], 0.0)
            picked[j, k * quarter : (k + 1) * quarter] = value


def final_kernel(dims, corners, slot_ref, field, picked, fine, coarse_out, fine_out, group, sems):
    nx, ny, nz, bx, by, bz = dims
    ix, iy, iz = lax.axis_index("gx"), lax.axis_index("gy"), lax.axis_index("gz")
    me = (ix * ny + iy) * nz + iz
    _, _, _, brick, place = grid_tables((bx, by, bz), ny, nz, corners, slot_ref)
    code = pick(brick == me, place)
    present = code >= 0
    code = jnp.maximum(code, 0)
    y_group = lax.div(lax.div(code, bz), B)
    z = lax.rem(code, bz)
    fine_copy = pltpu.make_async_copy(fine, fine_out, sems.at[0])
    fine_copy.start()

    def plain(g):
        return pltpu.make_async_copy(
            field.at[:, pl.ds(g * B, B)], coarse_out.at[:, pl.ds(g * B, B)], sems.at[1 + g]
        )

    def patched(g):
        return pltpu.make_async_copy(group, coarse_out.at[:, pl.ds(g * B, B)], sems.at[1 + g])

    for g in range(by // B):

        @pl.when(y_group != g)
        def _():
            plain(g).start()

    start = pl.multiple_of(y_group * B, B)
    low = lax.rem(z, LANES)
    tile = lax.div(z, LANES)
    lane = lax.broadcasted_iota(jnp.int32, (B, LANES), 1)
    eight = lane // B
    line = lax.broadcasted_iota(jnp.int32, (B, LANES), 0)
    chosen = eight % B == line
    first_half = (eight - line + 16) % 16 < B
    inside = [(lane >= low) & (lane < low + B) & (tile == t) & present for t in range(bz // LANES)]
    for j in range(SLOTS):
        for at in range(MEAN_ROWS):
            value = jnp.where(chosen, jnp.broadcast_to(picked[j, at : at + 1], (B, LANES)), 0.0)
            for step in (B, 2 * B, 4 * B):
                value += pltpu.roll(value, step, 1)
            swapped = pltpu.roll(value, 64, 1)
            k, a = at // (B // 2), at % (B // 2)
            for h in range(2):
                new = jnp.where(first_half, value, swapped) if h == 0 else jnp.where(first_half, swapped, value)
                x = k * bx + j * B + h * (B // 2) + a
                for t in range(bz // LANES):
                    old = field[x, pl.ds(start, B), t * LANES : (t + 1) * LANES]
                    group[x, :, t * LANES : (t + 1) * LANES] = jnp.where(inside[t], new, old)
    patched(y_group).start()
    for g in range(by // B):
        patched(g).wait()
    fine_copy.wait()


def on_device(coarse_field, fine_field, viscosity, corners, grid_slot, neighbors):
    nx, ny, nz = (lax.axis_size(n) for n in ("gx", "gy", "gz"))
    assert nz == 2
    bx, by, bz = coarse_field.shape[1:]
    dims = (nx, ny, nz, bx, by, bz)
    consts = matrices()
    vmem = pl.BlockSpec(memory_space=pltpu.VMEM)
    hbm = pl.BlockSpec(memory_space=pltpu.HBM)
    stay = functools.partial(pltpu.with_memory_space_constraint, memory_space=pltpu.HBM)
    grids = grid_slot.shape[0]
    f32 = jnp.float32
    dma = pltpu.SemaphoreType.DMA
    w_rows = bx + bx // 2 + 16
    planes = (IFACES, PLANE_LINES, F * F)
    means = (SLOTS, MEAN_ROWS, LANES)
    rims = (SLOTS // 2, F, LANES)
    tables_in = (corners.T, grid_slot.reshape(1, -1))
    fine_new, picked = pl.pallas_call(
        functools.partial(step_kernel, dims),
        out_shape=(
            jax.ShapeDtypeStruct(fine_field.shape, f32),
            jax.ShapeDtypeStruct((SLOTS, MEAN_ROWS, LANES), f32),
        ),
        in_specs=[hbm] * (6 + len(consts)),
        out_specs=(vmem, vmem),
        scratch_shapes=[
            pltpu.VMEM((3, grids), jnp.int32),
            pltpu.VMEM((1, grids), jnp.int32),
            pltpu.VMEM((2, grids), jnp.int32),
            pltpu.VMEM((bz // LANES, 3 * bx, by + 8, LANES), f32),
            pltpu.VMEM(fine_field.shape, f32),
            pltpu.VMEM(viscosity.shape, f32),
        ]
        + [pltpu.VMEM(c.shape, c.dtype) for c in consts]
        + [
            pltpu.VMEM(shape, f32)
            for shape in (
                (3, bx + 8, LANES),
                (w_rows, LANES),
                (w_rows, LANES),
                (ny, w_rows, LANES),
                (ny, *planes),
                (nx, *planes),
                (nx, *planes),
                (nx, *planes),
                (nx, E_ROWS, LANES),
                (nx, E_ROWS, LANES),
                (2, 3 * SLOTS * F, LANES),
                means,
                (nx, *means),
                rims,
                (nx, *rims),
                (ny, *means),
                (ny, *means),
                (ny, *rims),
                (ny, *rims),
                (ny, 2 * SLOTS, PLANE_LINES, F * F),
                (ny, 2 * SLOTS, PLANE_LINES, F * F),
            )
        ]
        + [
            dma((12 + bz // LANES,)),
            dma((2,)),
            dma((5, ny - 1)),
            dma((5, ny - 1)),
            dma((5, nx - 1)),
            dma((5, nx - 1)),
        ],
        compiler_params=pltpu.CompilerParams(collective_id=0, has_side_effects=True, vmem_limit_bytes=24 * MIB),
        name="step",
    )(
        *map(
            stay, (*tables_in, neighbors.T, coarse_field.reshape(3 * bx, by, bz), fine_field, viscosity, *consts)
        )
    )
    coarse_out, fine_out = pl.pallas_call(
        functools.partial(final_kernel, dims),
        out_shape=(
            jax.ShapeDtypeStruct((3 * bx, by, bz), f32),
            jax.ShapeDtypeStruct(fine_field.shape, f32),
        ),
        in_specs=[vmem] * 5,
        out_specs=(hbm, hbm),
        scratch_shapes=[pltpu.VMEM((3 * bx, B, bz), f32), dma((1 + by // B,))],
        compiler_params=pltpu.CompilerParams(vmem_limit_bytes=16 * MIB),
        name="final",
    )(*tables_in, coarse_field.reshape(3 * bx, by, bz), picked, fine_new)
    return fine_out, coarse_out.reshape(coarse_field.shape)


def solution(mesh):
    in_specs = (
        P(None, "gx", "gy", "gz"),
        P(None, ("gx", "gy", "gz"), None, None),
        P(("gx", "gy", "gz"), None, None),
        P(),
        P(),
        P(),
    )
    out_specs = (P(None, ("gx", "gy", "gz"), None, None), P(None, "gx", "gy", "gz"))
    return jax.shard_map(
        on_device, mesh=mesh, in_specs=in_specs, out_specs=out_specs, check_vma=False
    )
```

```python
import functools
import numpy as np
import jax
import jax.numpy as jnp
from jax import lax
from jax.experimental import pallas as pl
from jax.experimental.pallas import tpu as pltpu
from jax.sharding import PartitionSpec as P

B = 8
F = 16
SLOTS = 4
SIDE = B + 2
LANES = 128
WIDE = 4 * SIDE
IFACES = SLOTS + 1
PLANE_LINES = 4
FACES = 12
E_ROWS = 44
MEAN_ROWS = 12
step_rate = 0.15
MIB = 1 << 20


def tables():
    tangent = np.zeros((F, SIDE), np.float32)
    for f in range(F):
        c = f // 2 + 1
        tangent[f, c] = 0.75
        tangent[f, c - 1 if f % 2 == 0 else c + 1] = 0.25
    low = np.zeros((SIDE,), np.float32)
    low[0], low[1] = 0.75, 0.25
    return tangent, low, low[::-1].copy()


def matrices():
    tangent, low, high = tables()
    eye = np.eye(SIDE, dtype=np.float32)
    cut = np.zeros((SIDE, SIDE, 4, SIDE), np.float32)
    cut[:, :, 0] = np.einsum("b,cd->bcd", low, eye)
    cut[:, :, 1] = np.einsum("b,cd->bcd", high, eye)
    cut[:, :, 2] = np.einsum("bd,c->bcd", eye, low)
    cut[:, :, 3] = np.einsum("bd,c->bcd", eye, high)
    put = np.zeros((4, SIDE, F, F), np.float32)
    put[0, :, 0, :] = tangent.T
    put[1, :, F - 1, :] = tangent.T
    put[2, :, :, 0] = tangent.T
    put[3, :, :, F - 1] = tangent.T
    columns = np.zeros((3, LANES, LANES), np.float32)
    lines = np.zeros((LANES, 8, LANES), np.float32)
    ghost = np.zeros((LANES, 4, F * F), np.float32)
    for k in range(3):
        columns[k, : SIDE * SIDE, k * WIDE : (k + 1) * WIDE] = cut.reshape(SIDE * SIDE, WIDE)
        ghost[k * WIDE : (k + 1) * WIDE, k] = put.reshape(WIDE, F * F)
        for half in range(2):
            for side in range(2):
                for c in range(SIDE):
                    lane = half * 64 + k * 2 * SIDE + side * SIDE + c
                    window = side * (SIDE - 1) * SIDE + c
                    lines[lane, half] = columns[k, window]
                    lines[lane, 2 + 2 * k + half, window] = 1.0
    ghost[: SIDE * SIDE, 3] = np.einsum("sb,tc->bcst", tangent, tangent).reshape(SIDE * SIDE, F * F)
    mean = np.zeros((F * F, LANES), np.float32)
    for y in range(F):
        for z in range(F):
            for half in range(2):
                mean[y * F + z, half * 64 + (y // 2) * B + z // 2] = 0.125
    rim = [y * F + z for y in range(F) for z in range(F) if y in (0, F - 1) or z in (0, F - 1)]
    take = np.zeros((F * F, LANES), np.float32)
    rim_ghost = np.zeros((LANES, 3, LANES), np.float32)
    rim_mean = np.zeros((LANES, LANES), np.float32)
    for m, at in enumerate(rim):
        for half in range(2):
            take[at, half * 64 + m] = 1.0
            rim_ghost[:, :, half * 64 + m] = ghost[:, :3, at]
            rim_mean[half * 64 + m, half * 64 + (at // F // 2) * B + at % F // 2] = 0.125
    shapes = (
        columns.reshape(3 * LANES, LANES), lines.reshape(LANES, 8 * LANES), ghost.reshape(LANES, 4 * F * F),
        mean, take, rim_ghost.reshape(LANES, 3 * LANES), rim_mean,
    )
    return tuple(jnp.asarray(a, jnp.bfloat16) for a in shapes)


def div(a, n):
    return lax.div(a, jnp.full_like(a, n))


def rem(a, n):
    return lax.rem(a, jnp.full_like(a, n))


def split(a):
    high = a.astype(jnp.bfloat16)
    return high, (a - high.astype(jnp.float32)).astype(jnp.bfloat16)


def dot(a, b):
    return jnp.dot(a, b, preferred_element_type=jnp.float32)


def exact_right(a, b):
    high, low = split(a)
    return dot(high, b) + dot(low, b)


def exact_left(a, b):
    a = a.astype(jnp.bfloat16)
    high, low = split(b)
    return dot(a, high) + dot(a, low)


def pick(mask, value):
    return jnp.max(jnp.where(mask, value, -1))


def as_float(cond):
    return jnp.where(cond, 1.0, 0.0).astype(jnp.float32)


def grid_tables(bricks, ny, nz, corners, slot_ref):
    x, y, z = corners[0:1, :], corners[1:2, :], corners[2:3, :]
    slot = slot_ref[...]
    brick = (div(x, bricks[0]) * ny + div(y, bricks[1])) * nz + div(z, bricks[2])
    place = rem(y, bricks[1]) * bricks[2] + rem(z, bricks[2])
    return x, y, slot, brick, place


def step_kernel(
    dims, corners_in, slot_in, near_in, coarse, fine_in, visc_in,
    columns_in, lines_in, ghost_in, mean_in, take_in, rim_ghost_in, rim_mean_in,
    fine_out, picked, field,
    corners, slot_ref, near_ref, fine, visc, columns, lines, ghost, mean, take, rim_ghost, rim_mean,
    window, z_send, z_recv, w_buf, p_own, f_buf, e_send, e_buf,
    advs, m_send, m_buf, c_send, c_buf, qm_send, qm_buf, qc_send, qc_buf, qf_send, qf_buf,
    local_sem, z_sem, y_send_sem, y_recv_sem, x_send_sem, x_recv_sem,
):
    nx, ny, nz, bx, by, bz = dims
    ix, iy, iz = lax.axis_index("gx"), lax.axis_index("gy"), lax.axis_index("gz")
    me = (ix * ny + iy) * nz + iz
    mesh_id = pl.DeviceIdType.MESH
    tiles = bz // LANES
    half = bx // 2
    pitch = by + 8

    pairs = [
        (corners_in, corners), (slot_in, slot_ref), (near_in, near_ref), (fine_in, fine), (visc_in, visc),
        (mean_in, mean), (take_in, take),
    ]
    for t in range(tiles):
        pairs.append((coarse.at[:, :, t * LANES : (t + 1) * LANES], field.at[t, :, 0:by]))
    pairs += [
        (columns_in, columns), (lines_in, lines), (ghost_in, ghost),
        (rim_ghost_in, rim_ghost), (rim_mean_in, rim_mean),
    ]
    loads = [pltpu.make_async_copy(src, dst, local_sem.at[i]) for i, (src, dst) in enumerate(pairs)]
    for load in loads:
        load.start()
    table_loads, field_loads = loads[:3], loads[7 : 7 + tiles]
    fine_load, visc_load, mean_load, take_load = loads[3:7]
    columns_load, lines_load, ghost_load, rim_ghost_load, rim_mean_load = loads[7 + tiles :]

    def y_peer(o):
        return lax.rem(iy + o, ny)

    def x_peer(o):
        return lax.rem(ix + o, nx)

    barrier = pltpu.get_barrier_semaphore()
    pl.semaphore_signal(barrier, inc=1, device_id={"gz": 1 - iz}, device_id_type=mesh_id)

    def greet_y(o, c):
        pl.semaphore_signal(barrier, inc=1, device_id={"gy": y_peer(o)}, device_id_type=mesh_id)
        return c

    def greet_x(o, c):
        pl.semaphore_signal(barrier, inc=1, device_id={"gx": x_peer(o)}, device_id_type=mesh_id)
        return c

    lax.fori_loop(1, ny, greet_y, 0)
    lax.fori_loop(1, nx, greet_x, 0)

    def y_copy(which, o, src, dst):
        return pltpu.make_async_remote_copy(
            src_ref=src, dst_ref=dst, send_sem=y_send_sem.at[which, o - 1], recv_sem=y_recv_sem.at[which, o - 1],
            device_id={"gy": y_peer(o)}, device_id_type=mesh_id,
        )

    def x_copy(which, o, src, dst):
        return pltpu.make_async_remote_copy(
            src_ref=src, dst_ref=dst, send_sem=x_send_sem.at[which, o - 1], recv_sem=x_recv_sem.at[which, o - 1],
            device_id={"gx": x_peer(o)}, device_id_type=mesh_id,
        )

    def run(count, makes, action):
        def body(o, c):
            for make in makes:
                getattr(make(o), action)()
            return c

        lax.fori_loop(1, count, body, 0)

    for load in table_loads:
        load.wait()
    gx_, gy_, slot, brick, place = grid_tables((bx, by, bz), ny, nz, corners, slot_ref)
    home = div(gx_, bx) * ny + div(gy_, by)
    box = div(rem(gx_, bx), B)
    dev = div(slot, SLOTS)
    count = slot.shape[1]
    g_row = lax.broadcasted_iota(jnp.int32, (count, count), 0)
    g_col = lax.broadcasted_iota(jnp.int32, (count, count), 1)
    slot_col = jnp.max(jnp.where(g_row == g_col, slot, -1), axis=1, keepdims=True)
    near_slot = []
    far_dev = []
    for side in range(2):
        m = jnp.max(jnp.where(g_row == near_ref[side : side + 1, :], slot_col, -1), axis=0, keepdims=True)
        near_slot.append(m)
        d = div(jnp.maximum(m, 0), SLOTS)
        far_dev.append(jnp.where((m >= 0) & (d != dev), d, -1))

    def anchor(ox, oy, gz):
        hx, hy = ix + ox, iy + oy
        inside = (hx >= 0) & (hx < nx) & (hy >= 0) & (hy < ny)
        code = jnp.maximum(pick(brick == jnp.where(inside, (hx * ny + hy) * nz + gz, -5), place), 0)
        return lax.div(code, bz), lax.rem(code, bz)

    mine = dev == me
    own_slot = [pick(mine & (box == j), rem(slot, SLOTS)) for j in range(SLOTS)]
    slots = []
    for s in range(SLOTS):
        here = slot == me * SLOTS + s
        b = pick(here, box)
        near = []
        for side in range(2):
            m = pick(here, near_slot[side])
            n = jnp.maximum(m, 0)
            d = lax.div(n, SLOTS)
            near.append((m >= 0, d == me, lax.rem(n, SLOTS), lax.rem(lax.div(d, nz), ny)))
        slots.append((b >= 0, jnp.maximum(b, 0), near))

    fine_load.wait()
    visc_load.wait()
    for i in range(IFACES):
        below = jnp.maximum(own_slot[max(i - 1, 0)], 0)
        above = jnp.maximum(own_slot[min(i, SLOTS - 1)], 0)
        for k in range(PLANE_LINES):
            def line(n, x):
                return fine[k, n, x : x + 1] if k < 3 else step_rate * visc[n, x : x + 1]

            if i == 0:
                value = line(above, 0)
            elif i == SLOTS:
                value = line(below, F - 1)
            else:
                value = jnp.where(own_slot[i - 1] >= 0, line(below, F - 1), line(above, 0))
            p_own[i, k : k + 1] = value
    pl.semaphore_wait(barrier, nx + ny - 1)

    def f_copy(o):
        return x_copy(0, o, p_own, f_buf.at[ix])

    run(nx, [f_copy], "start")
    f_buf[ix] = p_own[...]

    lane = lax.broadcasted_iota(jnp.int32, (F, F * F), 1)
    row = lax.broadcasted_iota(jnp.int32, (F, F * F), 0)
    lz = lane % F
    for s in range(SLOTS):
        cv = step_rate * visc[s]
        for k in range(3):
            v = fine[k, s]
            ends = []
            for side in range(2):
                has, is_local, n, _ = slots[s][2][side]
                x = (F - 1) * (1 - side)
                ends.append(fine[k, n][x : x + 1] * as_float(has & is_local))
            total = jnp.where(row == 0, ends[0], pltpu.roll(v, 1, 0))
            total += jnp.where(row == F - 1, ends[1], pltpu.roll(v, F - 1, 0))
            total += jnp.where(lane < F, 0.0, pltpu.roll(v, F, 1))
            total += jnp.where(lane >= F * F - F, 0.0, pltpu.roll(v, F * F - F, 1))
            total += jnp.where(lz == 0, 0.0, pltpu.roll(v, 1, 1))
            total += jnp.where(lz == F - 1, 0.0, pltpu.roll(v, F * F - 1, 1))
            at = (s * 3 + k) * F
            value = v + cv * (total - 6.0 * v)
            advs[0, at : at + F] = value[:, :LANES]
            advs[1, at : at + F] = value[:, LANES:]
    rows = 3 * SLOTS * F // 2
    mean_load.wait()
    sums = [advs[h, pl.ds(0, rows, 2)] + advs[h, pl.ds(1, rows, 2)] for h in range(2)]
    z = exact_right(jnp.concatenate(sums, axis=1), mean[...])
    quarter = B // 2
    lane_m = lax.broadcasted_iota(jnp.int32, (quarter, LANES), 1)
    for s in range(SLOTS):
        for k in range(3):
            at = (s * 3 + k) * B
            m_send[s, k * quarter : (k + 1) * quarter] = jnp.where(
                lane_m < 64, z[at : at + quarter], z[at + quarter : at + B]
            )
    take_load.wait()
    lane_f = lax.broadcasted_iota(jnp.int32, (F, LANES), 1)
    rims = exact_right(step_rate * visc[...].reshape(SLOTS * F, F * F), take[...])
    for s in range(SLOTS // 2):
        low, high = rims[s * F : (s + 1) * F], rims[(s + 2) * F : (s + 3) * F]
        c_send[s] = jnp.where(lane_f < 64, low, high)

    def m_copy(o):
        return x_copy(1, o, m_send, m_buf.at[ix])

    def c_copy(o):
        return x_copy(2, o, c_send, c_buf.at[ix])

    run(nx, [m_copy, c_copy], "start")
    m_buf[ix] = m_send[...]
    c_buf[ix] = c_send[...]

    anchors = [
        {(ox, oy): anchor(ox, oy, gz) for ox in (-1, 0, 1) for oy in (-1, 0, 1)} for gz in (1 - iz, iz)
    ]
    flat = field.reshape(tiles, 3 * bx * pitch, LANES)
    stride = bx * pitch
    lane1 = lax.broadcasted_iota(jnp.int32, (1, LANES), 1)
    lane_b = div(lane1, SIDE)
    lane_c = rem(lane1, SIDE)
    half_lane = rem(lane1, 64)
    half_c = rem(half_lane, SIDE)
    line_id = div(half_lane, SIDE)

    def shifted(z, same, start, size, step, to):
        def get(t):
            return flat[t, pl.ds(start, size, step)] if size > 1 else flat[t, pl.ds(start, 1)]

        z = lax.rem(z - 1 + bz, bz)
        tile, low = lax.div(z, LANES), lax.rem(z, LANES)
        if same:
            lane = lax.broadcasted_iota(jnp.int32, (size, LANES), 1)
            value = jnp.where(lane >= low, get(tile), get(lax.rem(tile + 1, tiles)))
        else:
            value = get((tiles - 1) * (1 - iz))
        return pltpu.roll(value, lax.rem(to - low + LANES, LANES), 1)

    def z_weight(z, ids, same):
        first, last = z == 0, z == bz - B
        if same:
            return jnp.where(ids == 0, as_float(~first), jnp.where(ids == SIDE - 1, as_float(~last), 1.0))
        first = as_float(first & (iz == 0))
        last = as_float(last & (iz == 1))
        return jnp.where(ids == 0, first, jnp.where(ids == SIDE - 1, last, 0.0))

    def weights(y, z, same):
        weight = z_weight(z, lane_c, same)
        weight = weight * jnp.where(
            lane_b == 0, as_float(y > 0), jnp.where(lane_b == SIDE - 1, as_float(y < by - B), 1.0)
        )
        return jnp.where(lane1 < SIDE * SIDE, weight, 0.0)

    edge_at = bx + half
    line_at = edge_at + 2
    inner_at = line_at + 2
    outer_at = inner_at + 6

    def pack(place, same, to_ref):
        y, z = place[0, 0]
        weight = weights(y, z, same)
        for k in range(3):
            acc = jnp.zeros((bx, LANES), jnp.float32)
            for b in range(SIDE):
                at = jnp.clip(y - 1 + b, 0, by - 1)
                value = shifted(z, same, k * stride + at, bx, pitch, SIDE * b)
                acc = jnp.where(lane_b == b, value, acc)
            window[k, 0:bx] = acc * weight
        for n, ox in enumerate((1, -1)):
            y, z = place[ox, 0]
            weight = weights(y, z, same)
            x = bx - 1 if ox > 0 else 0
            acc = jnp.zeros((3, LANES), jnp.float32)
            for b in range(SIDE):
                at = jnp.clip(y - 1 + b, 0, by - 1)
                acc = jnp.where(lane_b == b, shifted(z, same, x * pitch + at, 3, stride, SIDE * b), acc)
            acc = acc * weight
            for k in range(3):
                window[k, bx + n : bx + n + 1] = acc[k : k + 1]
        total = jnp.zeros((bx + 8, LANES), jnp.float32)
        for k in range(3):
            total += exact_right(window[k], columns[k * LANES : (k + 1) * LANES])
            for side in range(2):
                at = inner_at + 2 * k + side
                inner = 0 if side == 0 else bx - 1
                to_ref[at : at + 1] = window[k, inner : inner + 1]
                to_ref[at + 6 : at + 7] = window[k, bx + side : bx + side + 1]
        to_ref[0:bx] = total[0:bx]
        to_ref[edge_at : edge_at + 2] = total[bx : bx + 2]
        main = [jnp.zeros((half, LANES), jnp.float32) for _ in range(2)]
        ends = [jnp.zeros((1, LANES), jnp.float32) for _ in range(2)]
        for side, oy in enumerate((1, -1)):
            at = by - 1 if oy > 0 else 0
            edge = 0 if oy > 0 else by - B
            y, z = place[0, oy]
            weight = z_weight(z, half_c, same) * as_float(y == edge)
            for k in range(3):
                to = k * 2 * SIDE + side * SIDE
                for h in range(2):
                    value = shifted(z, same, k * stride + h * half * pitch + at, half, pitch, to + 64 * h)
                    main[h] = jnp.where(line_id == 2 * k + side, value * weight, main[h])
            for n, ox in enumerate((1, -1)):
                y, z = place[ox, oy]
                weight = z_weight(z, half_c, same) * as_float(y == edge)
                x = bx - 1 if ox > 0 else 0
                for k in range(3):
                    to = k * 2 * SIDE + side * SIDE
                    value = shifted(z, same, k * stride + x * pitch + at, 1, 1, to)
                    ends[n] = jnp.where(line_id == 2 * k + side, value * weight, ends[n])
        to_ref[bx:edge_at] = jnp.where(lane1 < 64, main[0], main[1])
        for n in range(2):
            to_ref[line_at + n : line_at + n + 1] = jnp.where(lane1 < 64, ends[n], 0.0)

    own = w_buf.at[iy]
    for k in range(3):
        window[k, bx + 2 : bx + 8] = jnp.zeros((6, LANES), jnp.float32)
    for load in field_loads:
        load.wait()
    columns_load.wait()
    pack(anchors[0], False, z_send)
    z_copy = pltpu.make_async_remote_copy(
        src_ref=z_send, dst_ref=z_recv, send_sem=z_sem.at[0], recv_sem=z_sem.at[1],
        device_id={"gz": 1 - iz}, device_id_type=mesh_id,
    )
    z_copy.start()
    pack(anchors[1], True, own)
    z_copy.wait()
    own[...] += z_recv[...]

    def w_copy(o):
        return y_copy(0, o, own, own)

    run(ny, [w_copy], "start")

    homes = [pick(dev == (t * ny + iy) * nz + iz, home) for t in range(nx)]

    def brick_plan(t):
        here = brick == (ix * ny + t) * nz + iz
        held = [pick(here & (box == j), slot) for j in range(SLOTS)]
        low = pick(here & (box == 0), near_slot[0])
        high = pick(here & (box == SLOTS - 1), near_slot[1])
        near = [(held[j - 1] if j > 0 else low, held[j + 1] if j < SLOTS - 1 else high) for j in range(SLOTS)]
        return [jnp.maximum(n, 0) for n in held], near

    bricks = [brick_plan(t) for t in range(ny)]
    own_held, own_near = brick_plan(iy)

    side_x = SLOTS * nz * ny
    sources = []
    for t in range(ny):
        there = dev == (ix * ny + t) * nz + iz
        codes = []
        for i in range(IFACES):
            code = jnp.where(there & (box == i), far_dev[0], jnp.where(there & (box == i - 1), far_dev[1], -1))
            codes.append(lax.div(jnp.maximum(jnp.max(code), 0), nz * ny))
        sources.append(codes)
    run(nx, [f_copy], "wait")
    for t in range(ny):
        held, near = bricks[t]
        for j in range(SLOTS):
            tx = lax.div(held[j], side_x)
            for side in range(2):
                other = lax.div(jnp.maximum(near[j][side], 0), side_x)
                if side == 0:
                    at = j if j > 0 else SLOTS
                else:
                    at = j + 1 if j < SLOTS - 1 else 0
                qf_send[t, 2 * j + side, 0:3] = f_buf[other, at, 0:3]
                qf_send[t, 2 * j + side, 3:4] = f_buf[tx, j + side, 3:4]
        for i in range(IFACES):
            at = SLOTS if i == 0 else (0 if i == SLOTS else i)
            for k in range(3):
                n = 3 * i + k
                qf_send[t, 2 * SLOTS + n // 4, n % 4 : n % 4 + 1] = f_buf[sources[t][i], at, k : k + 1]
        qf_send[t, FACES - 1, 3:4] = jnp.zeros((1, F * F), jnp.float32)
    qf_buf[iy] = qf_send[iy]

    def qf_copy(o):
        return y_copy(3, o, qf_send.at[y_peer(o)], qf_buf.at[iy])

    run(ny, [qf_copy], "start")

    run(ny, [w_copy], "wait")
    lines_load.wait()
    low_line = rem(line_id, 2) == 0
    target_home = [jnp.maximum(h, 0) for h in homes]
    target_x = [lax.div(h, ny) for h in target_home] + [ix]
    target_y = [lax.rem(h, ny) for h in target_home] + [iy]
    mixed = []
    for hy in target_y:
        before, after = jnp.maximum(hy - 1, 0), jnp.minimum(hy + 1, ny - 1)
        low_on, high_on = as_float(hy > 0), as_float(hy < ny - 1)
        for first, last in ((bx, edge_at), (line_at, line_at + 2)):
            low, high = w_buf[before, first:last] * low_on, w_buf[after, first:last] * high_on
            mixed.append(jnp.where(low_line, low, high))
        mixed.append(jnp.zeros((6, LANES), jnp.float32))
    extras = exact_right(jnp.concatenate(mixed, axis=0), lines[...])

    def assemble(n):
        hy = target_y[n]
        extra = extras[n * (half + 8) : (n + 1) * (half + 8)]
        base = w_buf[hy]
        main = (base[0:half] + extra[0:half, 0:LANES], base[half:bx] + extra[0:half, LANES : 2 * LANES])
        ends = base[edge_at : edge_at + 2] + extra[half : half + 2, 0:LANES]
        inner, outer = {}, {}
        for k in range(3):
            for side in range(2):
                at = inner_at + 2 * k + side
                first = (2 + 2 * k + side) * LANES
                from_row = 0 if side == 0 else half - 1
                inner[k, side] = base[at : at + 1] + extra[from_row : from_row + 1, first : first + LANES]
                first = (2 + 2 * k) * LANES
                outer[k, side] = base[at + 6 : at + 7] + extra[half + side : half + side + 1, first : first + LANES]
        return main, ends, inner, outer

    home_main, home_ends, home_inner, home_outer = assemble(nx)
    for t in range(nx):
        main, ends, inner, outer = assemble(t)
        d = target_x[t] - ix
        same, up_one, down_one = as_float(d == 0), as_float(d == 1), as_float(d == -1)
        e_send[t, 0:half] = main[0] * same
        e_send[t, half:bx] = main[1] * same
        e_send[t, bx : bx + 1] = ends[0:1] * up_one
        e_send[t, bx + 1 : bx + 2] = ends[1:2] * down_one
        for k in range(3):
            for side in range(2):
                at = bx + 2 + 2 * k + side
                e_send[t, at : at + 1] = inner[k, side] * (0.25 * same) + outer[k, side] * (
                    0.75 * (down_one if side else up_one)
                )
        above = ix < t
        at = bx + 8
        e_send[t, at : at + 1] = jnp.where(above, home_ends[0:1], home_ends[1:2])
        for k in range(3):
            e_send[t, at + 1 + k : at + 2 + k] = 0.75 * jnp.where(above, home_outer[k, 0], home_outer[k, 1])
    e_buf[ix] = e_send[ix]

    def e_copy(o):
        return x_copy(3, o, e_send.at[x_peer(o)], e_buf.at[ix])

    run(nx, [e_copy], "start")

    run(nx, [m_copy, c_copy], "wait")
    for t in range(ny):
        held = bricks[t][0]
        for j in range(SLOTS):
            n = held[j]
            tx, s = lax.div(n, side_x), lax.rem(n, SLOTS)
            qm_send[t, j] = m_buf[tx, s]
            rim = c_buf[tx, lax.rem(s, 2)]
            flip = lax.div(s, 2) != j // 2
            rim = jnp.where(flip, pltpu.roll(rim, 64, 1), rim)
            keep = lane_f < 64 if j < 2 else lane_f >= 64
            if j < 2:
                qc_send[t, j] = rim
            else:
                qc_send[t, j % 2] = jnp.where(keep, rim, qc_send[t, j % 2])
    qm_buf[iy] = qm_send[iy]
    qc_buf[iy] = qc_send[iy]

    def qm_copy(o):
        return y_copy(1, o, qm_send.at[y_peer(o)], qm_buf.at[iy])

    def qc_copy(o):
        return y_copy(2, o, qc_send.at[y_peer(o)], qc_buf.at[iy])

    run(ny, [qc_copy, qm_copy], "start")

    def blended(boxes_of):
        shape = (SLOTS * F, bx + 8)
        out_line = lax.broadcasted_iota(jnp.int32, shape, 0)
        from_line = lax.broadcasted_iota(jnp.int32, shape, 1)
        boxes = jnp.full(shape, boxes_of[0], jnp.int32)
        for s in range(1, SLOTS):
            boxes = jnp.where(out_line // F == s, boxes_of[s], boxes)
        f_id = out_line % F
        center = B * boxes + f_id // 2
        other = jnp.where(f_id % 2 == 0, center - 1, center + 1)
        other = jnp.where(other < 0, bx, jnp.where(other >= bx, bx + 1, other))
        return jnp.where(from_line == center, 0.75, jnp.where(from_line == other, 0.25, 0.0))

    blend = blended([slots[s][1] for s in range(SLOTS)])
    home_blend = blended(list(range(SLOTS)))
    for load in (ghost_load, rim_ghost_load, rim_mean_load):
        load.wait()
    run(nx, [e_copy], "wait")
    run(ny, [qf_copy], "wait")
    total = e_buf[0, 0 : bx + 8]
    for t in range(1, nx):
        total += e_buf[t, 0 : bx + 8]
    along = exact_left(blend, total)
    ghosts = exact_right(along, ghost[:, 0 : 3 * F * F])
    faces = exact_right(total[bx : bx + 8], ghost[:, 3 * F * F :])
    for s in range(SLOTS):
        active, b, near = slots[s]
        cv = step_rate * visc[s]
        for k in range(3):
            ends = []
            for side in range(2):
                has, is_local, _, sy = near[side]
                n = 3 * (b + side) + k
                far = qf_buf[sy, 2 * SLOTS + lax.div(n, 4), pl.ds(lax.rem(n, 4), 1)]
                outer = faces[2 + 2 * k + side : 3 + 2 * k + side]
                ends.append(jnp.where(has, far * as_float(~is_local), outer))
            edge = jnp.where(row == 0, ends[0], jnp.where(row == F - 1, ends[1], 0.0))
            at = (s * 3 + k) * F
            ghost_k = ghosts[s * F : s * F + F, k * F * F : (k + 1) * F * F]
            adv = jnp.concatenate([advs[0, at : at + F], advs[1, at : at + F]], axis=1) + cv * (ghost_k + edge)
            fine_out[k, s] = jnp.where(active, adv, 0.0)

    before = e_buf[jnp.maximum(ix - 1, 0), bx + 8 : E_ROWS] * as_float(ix > 0)
    after = e_buf[jnp.minimum(ix + 1, nx - 1), bx + 8 : E_ROWS] * as_float(ix < nx - 1)
    face_lines = []
    for k in range(3):
        for side in range(2):
            far = after if side else before
            face_lines.append(0.25 * home_inner[k, side] + far[1 + k : 2 + k])
    home_total = jnp.concatenate([*home_main, before[0:1], after[0:1], *face_lines], axis=0)
    home_along = exact_left(home_blend, home_total)
    rim_ghosts = exact_right(home_along, rim_ghost[...])
    home_faces = exact_right(home_total[bx : bx + 8], ghost[:, 3 * F * F :])
    run(ny, [qc_copy, qm_copy], "wait")

    def row_of(n):
        return lax.rem(lax.div(jnp.maximum(n, 0), SLOTS * nz), ny)

    x_lines = []
    for j in range(SLOTS):
        own_row = row_of(own_held[j])
        own_dev = lax.div(own_held[j], SLOTS)
        for side in range(2):
            m = own_near[j][side]
            other_dev = lax.div(jnp.maximum(m, 0), SLOTS)
            on = as_float((m < 0) | (own_dev != other_dev))
            weight = qf_buf[own_row, 2 * j + side, 3:4] * on
            for k in range(3):
                far = qf_buf[row_of(m), 2 * j + side, k : k + 1]
                x_lines.append(weight * jnp.where(m >= 0, far, home_faces[2 + 2 * k + side : 3 + 2 * k + side]))
    x_means = exact_right(jnp.concatenate(x_lines, axis=0), mean[...])
    products = []
    for j in range(SLOTS // 2):
        low = qc_buf[row_of(own_held[j]), j]
        high = qc_buf[row_of(own_held[j + 2]), j]
        rim = jnp.where(lane_f < 64, low, high)
        for k in range(3):
            low = rim_ghosts[j * F : (j + 1) * F, k * LANES : (k + 1) * LANES]
            high = rim_ghosts[(j + 2) * F : (j + 3) * F, k * LANES : (k + 1) * LANES]
            window[(3 * j + k) // 2, (3 * j + k) % 2 * F : (3 * j + k) % 2 * F + F] = rim * jnp.where(
                lane_f < 64, low, high
            )
    for n in range(3):
        products.append(window[n, pl.ds(0, F, 2)] + window[n, pl.ds(1, F, 2)])
    rim_means = exact_right(jnp.concatenate(products, axis=0), rim_mean[...])
    for j in range(SLOTS):
        own_row = row_of(own_held[j])
        for k in range(3):
            at = (3 * (j % 2) + k) * B
            low, high = rim_means[at : at + quarter], rim_means[at + quarter : at + B]
            if j < 2:
                high = pltpu.roll(high, 64, 1)
            else:
                low = pltpu.roll(low, 64, 1)
            value = qm_buf[own_row, j, k * quarter : (k + 1) * quarter] + jnp.where(lane_m < 64, low, high)
            row_m = lax.broadcasted_iota(jnp.int32, (quarter, LANES), 0)
            for side in range(2):
                n = (2 * j + side) * 3 + k
                place = (row_m == 0) & (lane_m < 64) if side == 0 else (row_m == quarter - 1) & (lane_m >= 64)
                value += jnp.where(place, x_means[n : n + 1], 0.0)
            picked[j, k * quarter : (k + 1) * quarter] = value


def final_kernel(dims, corners, slot_ref, field, picked, fine, coarse_out, fine_out, group, sems):
    nx, ny, nz, bx, by, bz = dims
    ix, iy, iz = lax.axis_index("gx"), lax.axis_index("gy"), lax.axis_index("gz")
    me = (ix * ny + iy) * nz + iz
    _, _, _, brick, place = grid_tables((bx, by, bz), ny, nz, corners, slot_ref)
    code = pick(brick == me, place)
    present = code >= 0
    code = jnp.maximum(code, 0)
    y_group = lax.div(lax.div(code, bz), B)
    z = lax.rem(code, bz)
    tiles = bz // LANES
    low = lax.rem(z, LANES)
    tile = lax.div(z, LANES)
    fine_copy = pltpu.make_async_copy(fine, fine_out, sems.at[0, 0])

    def at(g, t):
        return coarse_out.at[:, pl.ds(pl.multiple_of(g * B, B), B), pl.ds(pl.multiple_of(t * LANES, LANES), LANES)]

    def plain(g, t):
        return pltpu.make_async_copy(field.at[t, :, g * B : (g + 1) * B], at(g, t), sems.at[1 + g, t])

    def patched(g, t):
        return pltpu.make_async_copy(group, at(g, t), sems.at[1 + g, t])

    for g in range(by // B):
        for t in range(tiles):

            @pl.when((y_group != g) | (tile != t))
            def _():
                plain(g, t).start()

    fine_copy.start()
    start = pl.multiple_of(y_group * B, B)
    lane = lax.broadcasted_iota(jnp.int32, (B, LANES), 1)
    eight = lane // B
    line = lax.broadcasted_iota(jnp.int32, (B, LANES), 0)
    chosen = eight % B == line
    first_half = (eight - line + 16) % 16 < B
    inside = (lane >= low) & (lane < low + B) & present
    for j in range(SLOTS):
        for row in range(MEAN_ROWS):
            value = jnp.where(chosen, jnp.broadcast_to(picked[j, row : row + 1], (B, LANES)), 0.0)
            for step in (B, 2 * B, 4 * B):
                value += pltpu.roll(value, step, 1)
            swapped = pltpu.roll(value, 64, 1)
            k, a = row // (B // 2), row % (B // 2)
            for h in range(2):
                new = jnp.where(first_half, value, swapped) if h == 0 else jnp.where(first_half, swapped, value)
                x = k * bx + j * B + h * (B // 2) + a
                group[x] = jnp.where(inside, new, field[tile, x, pl.ds(start, B)])
    patched(y_group, tile).start()
    for g in range(by // B):
        for t in range(tiles):
            patched(g, t).wait()
    fine_copy.wait()


def on_device(coarse_field, fine_field, viscosity, corners, grid_slot, neighbors):
    nx, ny, nz = (lax.axis_size(n) for n in ("gx", "gy", "gz"))
    assert nz == 2
    bx, by, bz = coarse_field.shape[1:]
    dims = (nx, ny, nz, bx, by, bz)
    consts = matrices()
    vmem = pl.BlockSpec(memory_space=pltpu.VMEM)
    hbm = pl.BlockSpec(memory_space=pltpu.HBM)
    stay = functools.partial(pltpu.with_memory_space_constraint, memory_space=pltpu.HBM)
    grids = grid_slot.shape[0]
    f32 = jnp.float32
    dma = pltpu.SemaphoreType.DMA
    w_rows = bx + bx // 2 + 16
    planes = (IFACES, PLANE_LINES, F * F)
    means = (SLOTS, MEAN_ROWS, LANES)
    rims = (SLOTS // 2, F, LANES)
    tables_in = (corners.T, grid_slot.reshape(1, -1))
    fine_new, picked, field = pl.pallas_call(
        functools.partial(step_kernel, dims),
        out_shape=(
            jax.ShapeDtypeStruct(fine_field.shape, f32),
            jax.ShapeDtypeStruct((SLOTS, MEAN_ROWS, LANES), f32),
            jax.ShapeDtypeStruct((bz // LANES, 3 * bx, by + 8, LANES), f32),
        ),
        in_specs=[hbm] * (6 + len(consts)),
        out_specs=(vmem, vmem, vmem),
        scratch_shapes=[
            pltpu.VMEM((3, grids), jnp.int32),
            pltpu.VMEM((1, grids), jnp.int32),
            pltpu.VMEM((2, grids), jnp.int32),
            pltpu.VMEM(fine_field.shape, f32),
            pltpu.VMEM(viscosity.shape, f32),
        ]
        + [pltpu.VMEM(c.shape, c.dtype) for c in consts]
        + [
            pltpu.VMEM(shape, f32)
            for shape in (
                (3, bx + 8, LANES),
                (w_rows, LANES),
                (w_rows, LANES),
                (ny, w_rows, LANES),
                planes,
                (nx, *planes),
                (nx, E_ROWS, LANES),
                (nx, E_ROWS, LANES),
                (2, 3 * SLOTS * F, LANES),
                means,
                (nx, *means),
                rims,
                (nx, *rims),
                (ny, *means),
                (ny, *means),
                (ny, *rims),
                (ny, *rims),
                (ny, FACES, PLANE_LINES, F * F),
                (ny, FACES, PLANE_LINES, F * F),
            )
        ]
        + [
            dma((12 + bz // LANES,)),
            dma((2,)),
            dma((4, ny - 1)),
            dma((4, ny - 1)),
            dma((4, nx - 1)),
            dma((4, nx - 1)),
        ],
        compiler_params=pltpu.CompilerParams(collective_id=0, has_side_effects=True, vmem_limit_bytes=24 * MIB),
        name="step",
    )(
        *map(
            stay, (*tables_in, neighbors.T, coarse_field.reshape(3 * bx, by, bz), fine_field, viscosity, *consts)
        )
    )
    coarse_out, fine_out = pl.pallas_call(
        functools.partial(final_kernel, dims),
        out_shape=(
            jax.ShapeDtypeStruct((3 * bx, by, bz), f32),
            jax.ShapeDtypeStruct(fine_field.shape, f32),
        ),
        in_specs=[vmem] * 5,
        out_specs=(hbm, hbm),
        scratch_shapes=[pltpu.VMEM((3 * bx, B, LANES), f32), dma((1 + by // B, bz // LANES))],
        compiler_params=pltpu.CompilerParams(vmem_limit_bytes=16 * MIB),
        name="final",
    )(*tables_in, field, picked, fine_new)
    return fine_out, coarse_out.reshape(coarse_field.shape)


def solution(mesh):
    in_specs = (
        P(None, "gx", "gy", "gz"),
        P(None, ("gx", "gy", "gz"), None, None),
        P(("gx", "gy", "gz"), None, None),
        P(),
        P(),
        P(),
    )
    out_specs = (P(None, ("gx", "gy", "gz"), None, None), P(None, "gx", "gy", "gz"))
    return jax.shard_map(
        on_device, mesh=mesh, in_specs=in_specs, out_specs=out_specs, check_vma=False
    )
```

```python
import functools
import numpy as np
import jax
import jax.numpy as jnp
from jax import lax
from jax.experimental import pallas as pl
from jax.experimental.pallas import tpu as pltpu
from jax.sharding import PartitionSpec as P

B = 8
F = 16
SLOTS = 4
SIDE = B + 2
LANES = 128
WIDE = 4 * SIDE
IFACES = SLOTS + 1
PLANE_LINES = 4
FACES = 12
E_ROWS = 44
MEAN_ROWS = 12
step_rate = 0.15
MIB = 1 << 20


def tables():
    tangent = np.zeros((F, SIDE), np.float32)
    for f in range(F):
        c = f // 2 + 1
        tangent[f, c] = 0.75
        tangent[f, c - 1 if f % 2 == 0 else c + 1] = 0.25
    low = np.zeros((SIDE,), np.float32)
    low[0], low[1] = 0.75, 0.25
    return tangent, low, low[::-1].copy()


def matrices():
    tangent, low, high = tables()
    eye = np.eye(SIDE, dtype=np.float32)
    cut = np.zeros((SIDE, SIDE, 4, SIDE), np.float32)
    cut[:, :, 0] = np.einsum("b,cd->bcd", low, eye)
    cut[:, :, 1] = np.einsum("b,cd->bcd", high, eye)
    cut[:, :, 2] = np.einsum("bd,c->bcd", eye, low)
    cut[:, :, 3] = np.einsum("bd,c->bcd", eye, high)
    put = np.zeros((4, SIDE, F, F), np.float32)
    put[0, :, 0, :] = tangent.T
    put[1, :, F - 1, :] = tangent.T
    put[2, :, :, 0] = tangent.T
    put[3, :, :, F - 1] = tangent.T
    columns = np.zeros((3, LANES, LANES), np.float32)
    lines = np.zeros((LANES, 8, LANES), np.float32)
    ghost = np.zeros((LANES, 4, F * F), np.float32)
    for k in range(3):
        columns[k, : SIDE * SIDE, k * WIDE : (k + 1) * WIDE] = cut.reshape(SIDE * SIDE, WIDE)
        ghost[k * WIDE : (k + 1) * WIDE, k] = put.reshape(WIDE, F * F)
        for half in range(2):
            for side in range(2):
                for c in range(SIDE):
                    lane = half * 64 + k * 2 * SIDE + side * SIDE + c
                    window = side * (SIDE - 1) * SIDE + c
                    lines[lane, half] = columns[k, window]
                    lines[lane, 2 + 2 * k + half, window] = 1.0
    ghost[: SIDE * SIDE, 3] = np.einsum("sb,tc->bcst", tangent, tangent).reshape(SIDE * SIDE, F * F)
    mean = np.zeros((F * F, LANES), np.float32)
    for y in range(F):
        for z in range(F):
            for half in range(2):
                mean[y * F + z, half * 64 + (y // 2) * B + z // 2] = 0.125
    rim = [y * F + z for y in range(F) for z in range(F) if y in (0, F - 1) or z in (0, F - 1)]
    take = np.zeros((F * F, LANES), np.float32)
    rim_ghost = np.zeros((LANES, 3, LANES), np.float32)
    rim_mean = np.zeros((LANES, LANES), np.float32)
    for m, at in enumerate(rim):
        for half in range(2):
            take[at, half * 64 + m] = 1.0
            rim_ghost[:, :, half * 64 + m] = ghost[:, :3, at]
            rim_mean[half * 64 + m, half * 64 + (at // F // 2) * B + at % F // 2] = 0.125
    shapes = (
        columns.reshape(3 * LANES, LANES), lines.reshape(LANES, 8 * LANES), ghost.reshape(LANES, 4 * F * F),
        mean, take, rim_ghost.reshape(LANES, 3 * LANES), rim_mean,
    )
    return tuple(jnp.asarray(a, jnp.bfloat16) for a in shapes)


def div(a, n):
    return lax.div(a, jnp.full_like(a, n))


def rem(a, n):
    return lax.rem(a, jnp.full_like(a, n))


def split(a):
    high = a.astype(jnp.bfloat16)
    return high, (a - high.astype(jnp.float32)).astype(jnp.bfloat16)


def dot(a, b):
    return jnp.dot(a, b, preferred_element_type=jnp.float32)


def exact_right(a, b):
    high, low = split(a)
    return dot(high, b) + dot(low, b)


def exact_left(a, b):
    a = a.astype(jnp.bfloat16)
    high, low = split(b)
    return dot(a, high) + dot(a, low)


def pick(mask, value):
    return jnp.max(jnp.where(mask, value, -1))


def as_float(cond):
    return jnp.where(cond, 1.0, 0.0).astype(jnp.float32)


def grid_tables(bricks, ny, nz, corners, slot_ref):
    x, y, z = corners[0:1, :], corners[1:2, :], corners[2:3, :]
    slot = slot_ref[...]
    brick = (div(x, bricks[0]) * ny + div(y, bricks[1])) * nz + div(z, bricks[2])
    place = rem(y, bricks[1]) * bricks[2] + rem(z, bricks[2])
    return x, y, slot, brick, place


def step_kernel(
    dims, corners_in, slot_in, near_in, coarse, fine_in, visc_in,
    columns_in, lines_in, ghost_in, mean_in, take_in, rim_ghost_in, rim_mean_in,
    fine_out, picked, field,
    corners, slot_ref, near_ref, fine, visc, columns, lines, ghost, mean, take, rim_ghost, rim_mean,
    window, z_send, z_recv, w_buf, p_own, f_buf, e_send, e_buf,
    advs, m_send, m_buf, c_send, c_buf, qm_send, qm_buf, qc_send, qc_buf, qf_send, qf_buf,
    local_sem, z_sem, y_send_sem, y_recv_sem, x_send_sem, x_recv_sem,
):
    nx, ny, nz, bx, by, bz = dims
    ix, iy, iz = lax.axis_index("gx"), lax.axis_index("gy"), lax.axis_index("gz")
    me = (ix * ny + iy) * nz + iz
    mesh_id = pl.DeviceIdType.MESH
    tiles = bz // LANES
    half = bx // 2
    pitch = by + 8

    pairs = [
        (corners_in, corners), (slot_in, slot_ref), (near_in, near_ref), (fine_in, fine), (visc_in, visc),
        (mean_in, mean), (take_in, take),
    ]
    for t in range(tiles):
        pairs.append((coarse.at[:, :, t * LANES : (t + 1) * LANES], field.at[t, :, 0:by]))
    pairs += [
        (columns_in, columns), (lines_in, lines), (ghost_in, ghost),
        (rim_ghost_in, rim_ghost), (rim_mean_in, rim_mean),
    ]
    loads = [pltpu.make_async_copy(src, dst, local_sem.at[i]) for i, (src, dst) in enumerate(pairs)]
    for load in loads:
        load.start()
    table_loads, field_loads = loads[:3], loads[7 : 7 + tiles]
    fine_load, visc_load, mean_load, take_load = loads[3:7]
    columns_load, lines_load, ghost_load, rim_ghost_load, rim_mean_load = loads[7 + tiles :]

    def y_peer(o):
        return lax.rem(iy + o, ny)

    def x_peer(o):
        return lax.rem(ix + o, nx)

    barrier = pltpu.get_barrier_semaphore()
    pl.semaphore_signal(barrier, inc=1, device_id={"gz": 1 - iz}, device_id_type=mesh_id)

    def greet_y(o, c):
        pl.semaphore_signal(barrier, inc=1, device_id={"gy": y_peer(o)}, device_id_type=mesh_id)
        return c

    def greet_x(o, c):
        pl.semaphore_signal(barrier, inc=1, device_id={"gx": x_peer(o)}, device_id_type=mesh_id)
        return c

    lax.fori_loop(1, ny, greet_y, 0)
    lax.fori_loop(1, nx, greet_x, 0)

    def y_copy(which, o, src, dst):
        return pltpu.make_async_remote_copy(
            src_ref=src, dst_ref=dst, send_sem=y_send_sem.at[which, o - 1], recv_sem=y_recv_sem.at[which, o - 1],
            device_id={"gy": y_peer(o)}, device_id_type=mesh_id,
        )

    def x_copy(which, o, src, dst):
        return pltpu.make_async_remote_copy(
            src_ref=src, dst_ref=dst, send_sem=x_send_sem.at[which, o - 1], recv_sem=x_recv_sem.at[which, o - 1],
            device_id={"gx": x_peer(o)}, device_id_type=mesh_id,
        )

    def run(count, makes, action):
        def body(o, c):
            for make in makes:
                getattr(make(o), action)()
            return c

        lax.fori_loop(1, count, body, 0)

    def run_if(cond, count, makes):
        @pl.when(cond)
        def _():
            run(count, makes, "start")

    for load in table_loads:
        load.wait()
    gx_, gy_, slot, brick, place = grid_tables((bx, by, bz), ny, nz, corners, slot_ref)
    home = div(gx_, bx) * ny + div(gy_, by)
    box = div(rem(gx_, bx), B)
    dev = div(slot, SLOTS)
    count = slot.shape[1]
    g_row = lax.broadcasted_iota(jnp.int32, (count, count), 0)
    g_col = lax.broadcasted_iota(jnp.int32, (count, count), 1)
    slot_col = jnp.max(jnp.where(g_row == g_col, slot, -1), axis=1, keepdims=True)
    near_slot = []
    far_dev = []
    for side in range(2):
        m = jnp.max(jnp.where(g_row == near_ref[side : side + 1, :], slot_col, -1), axis=0, keepdims=True)
        near_slot.append(m)
        d = div(jnp.maximum(m, 0), SLOTS)
        far_dev.append(jnp.where((m >= 0) & (d != dev), d, -1))

    def anchor(ox, oy, gz):
        hx, hy = ix + ox, iy + oy
        inside = (hx >= 0) & (hx < nx) & (hy >= 0) & (hy < ny)
        code = jnp.maximum(pick(brick == jnp.where(inside, (hx * ny + hy) * nz + gz, -5), place), 0)
        return lax.div(code, bz), lax.rem(code, bz)

    mine = dev == me
    own_slot = [pick(mine & (box == j), rem(slot, SLOTS)) for j in range(SLOTS)]
    slots = []
    for s in range(SLOTS):
        here = slot == me * SLOTS + s
        b = pick(here, box)
        near = []
        for side in range(2):
            m = pick(here, near_slot[side])
            n = jnp.maximum(m, 0)
            d = lax.div(n, SLOTS)
            near.append((m >= 0, d == me, lax.rem(n, SLOTS), lax.rem(lax.div(d, nz), ny)))
        slots.append((b >= 0, jnp.maximum(b, 0), near))

    fine_load.wait()
    visc_load.wait()
    for i in range(IFACES):
        below = jnp.maximum(own_slot[max(i - 1, 0)], 0)
        above = jnp.maximum(own_slot[min(i, SLOTS - 1)], 0)
        for k in range(PLANE_LINES):
            def line(n, x):
                return fine[k, n, x : x + 1] if k < 3 else step_rate * visc[n, x : x + 1]

            if i == 0:
                value = line(above, 0)
            elif i == SLOTS:
                value = line(below, F - 1)
            else:
                value = jnp.where(own_slot[i - 1] >= 0, line(below, F - 1), line(above, 0))
            p_own[i, k : k + 1] = value

    def f_copy(o):
        return x_copy(0, o, p_own, f_buf.at[ix])


    lane = lax.broadcasted_iota(jnp.int32, (F, F * F), 1)
    row = lax.broadcasted_iota(jnp.int32, (F, F * F), 0)
    lz = lane % F
    for s in range(SLOTS):
        cv = step_rate * visc[s]
        for k in range(3):
            v = fine[k, s]
            ends = []
            for side in range(2):
                has, is_local, n, _ = slots[s][2][side]
                x = (F - 1) * (1 - side)
                ends.append(fine[k, n][x : x + 1] * as_float(has & is_local))
            total = jnp.where(row == 0, ends[0], pltpu.roll(v, 1, 0))
            total += jnp.where(row == F - 1, ends[1], pltpu.roll(v, F - 1, 0))
            total += jnp.where(lane < F, 0.0, pltpu.roll(v, F, 1))
            total += jnp.where(lane >= F * F - F, 0.0, pltpu.roll(v, F * F - F, 1))
            total += jnp.where(lz == 0, 0.0, pltpu.roll(v, 1, 1))
            total += jnp.where(lz == F - 1, 0.0, pltpu.roll(v, F * F - 1, 1))
            at = (s * 3 + k) * F
            value = v + cv * (total - 6.0 * v)
            advs[0, at : at + F] = value[:, :LANES]
            advs[1, at : at + F] = value[:, LANES:]
    rows = 3 * SLOTS * F // 2
    mean_load.wait()
    sums = [advs[h, pl.ds(0, rows, 2)] + advs[h, pl.ds(1, rows, 2)] for h in range(2)]
    z = exact_right(jnp.concatenate(sums, axis=1), mean[...])
    quarter = B // 2
    lane_m = lax.broadcasted_iota(jnp.int32, (quarter, LANES), 1)
    for s in range(SLOTS):
        for k in range(3):
            at = (s * 3 + k) * B
            m_send[s, k * quarter : (k + 1) * quarter] = jnp.where(
                lane_m < 64, z[at : at + quarter], z[at + quarter : at + B]
            )
    def m_copy(o):
        return x_copy(1, o, m_send, m_buf.at[ix])

    pl.semaphore_wait(barrier, nx + ny - 1)
    run(nx, [f_copy], "start")
    run_if(iz == 1, nx, [m_copy])

    anchors = [
        {(ox, oy): anchor(ox, oy, gz) for ox in (-1, 0, 1) for oy in (-1, 0, 1)} for gz in (1 - iz, iz)
    ]
    flat = field.reshape(tiles, 3 * bx * pitch, LANES)
    stride = bx * pitch
    lane1 = lax.broadcasted_iota(jnp.int32, (1, LANES), 1)
    lane_b = div(lane1, SIDE)
    lane_c = rem(lane1, SIDE)
    half_lane = rem(lane1, 64)
    half_c = rem(half_lane, SIDE)
    line_id = div(half_lane, SIDE)

    def shifted(z, same, start, size, step, to):
        def get(t):
            return flat[t, pl.ds(start, size, step)] if size > 1 else flat[t, pl.ds(start, 1)]

        z = lax.rem(z - 1 + bz, bz)
        tile, low = lax.div(z, LANES), lax.rem(z, LANES)
        if same:
            lane = lax.broadcasted_iota(jnp.int32, (size, LANES), 1)
            value = jnp.where(lane >= low, get(tile), get(lax.rem(tile + 1, tiles)))
        else:
            value = get((tiles - 1) * (1 - iz))
        return pltpu.roll(value, lax.rem(to - low + LANES, LANES), 1)

    def z_weight(z, ids, same):
        first, last = z == 0, z == bz - B
        if same:
            return jnp.where(ids == 0, as_float(~first), jnp.where(ids == SIDE - 1, as_float(~last), 1.0))
        first = as_float(first & (iz == 0))
        last = as_float(last & (iz == 1))
        return jnp.where(ids == 0, first, jnp.where(ids == SIDE - 1, last, 0.0))

    def weights(y, z, same):
        weight = z_weight(z, lane_c, same)
        weight = weight * jnp.where(
            lane_b == 0, as_float(y > 0), jnp.where(lane_b == SIDE - 1, as_float(y < by - B), 1.0)
        )
        return jnp.where(lane1 < SIDE * SIDE, weight, 0.0)

    edge_at = bx + half
    line_at = edge_at + 2
    inner_at = line_at + 2
    outer_at = inner_at + 6

    def pack(place, same, to_ref):
        y, z = place[0, 0]
        weight = weights(y, z, same)
        for k in range(3):
            acc = jnp.zeros((bx, LANES), jnp.float32)
            for b in range(SIDE):
                at = jnp.clip(y - 1 + b, 0, by - 1)
                value = shifted(z, same, k * stride + at, bx, pitch, SIDE * b)
                acc = jnp.where(lane_b == b, value, acc)
            window[k, 0:bx] = acc * weight
        for n, ox in enumerate((1, -1)):
            y, z = place[ox, 0]
            weight = weights(y, z, same)
            x = bx - 1 if ox > 0 else 0
            acc = jnp.zeros((3, LANES), jnp.float32)
            for b in range(SIDE):
                at = jnp.clip(y - 1 + b, 0, by - 1)
                acc = jnp.where(lane_b == b, shifted(z, same, x * pitch + at, 3, stride, SIDE * b), acc)
            acc = acc * weight
            for k in range(3):
                window[k, bx + n : bx + n + 1] = acc[k : k + 1]
        total = jnp.zeros((bx + 8, LANES), jnp.float32)
        for k in range(3):
            total += exact_right(window[k], columns[k * LANES : (k + 1) * LANES])
            for side in range(2):
                at = inner_at + 2 * k + side
                inner = 0 if side == 0 else bx - 1
                to_ref[at : at + 1] = window[k, inner : inner + 1]
                to_ref[at + 6 : at + 7] = window[k, bx + side : bx + side + 1]
        to_ref[0:bx] = total[0:bx]
        to_ref[edge_at : edge_at + 2] = total[bx : bx + 2]
        main = [jnp.zeros((half, LANES), jnp.float32) for _ in range(2)]
        ends = [jnp.zeros((1, LANES), jnp.float32) for _ in range(2)]
        for side, oy in enumerate((1, -1)):
            at = by - 1 if oy > 0 else 0
            edge = 0 if oy > 0 else by - B
            y, z = place[0, oy]
            weight = z_weight(z, half_c, same) * as_float(y == edge)
            for k in range(3):
                to = k * 2 * SIDE + side * SIDE
                for h in range(2):
                    value = shifted(z, same, k * stride + h * half * pitch + at, half, pitch, to + 64 * h)
                    main[h] = jnp.where(line_id == 2 * k + side, value * weight, main[h])
            for n, ox in enumerate((1, -1)):
                y, z = place[ox, oy]
                weight = z_weight(z, half_c, same) * as_float(y == edge)
                x = bx - 1 if ox > 0 else 0
                for k in range(3):
                    to = k * 2 * SIDE + side * SIDE
                    value = shifted(z, same, k * stride + x * pitch + at, 1, 1, to)
                    ends[n] = jnp.where(line_id == 2 * k + side, value * weight, ends[n])
        to_ref[bx:edge_at] = jnp.where(lane1 < 64, main[0], main[1])
        for n in range(2):
            to_ref[line_at + n : line_at + n + 1] = jnp.where(lane1 < 64, ends[n], 0.0)

    own = w_buf.at[iy]
    for k in range(3):
        window[k, bx + 2 : bx + 8] = jnp.zeros((6, LANES), jnp.float32)
    for load in field_loads:
        load.wait()
    columns_load.wait()
    pack(anchors[0], False, z_send)
    z_copy = pltpu.make_async_remote_copy(
        src_ref=z_send, dst_ref=z_recv, send_sem=z_sem.at[0], recv_sem=z_sem.at[1],
        device_id={"gz": 1 - iz}, device_id_type=mesh_id,
    )
    z_copy.start()
    pack(anchors[1], True, own)
    take_load.wait()
    lane_f = lax.broadcasted_iota(jnp.int32, (F, LANES), 1)
    rims = exact_right(step_rate * visc[...].reshape(SLOTS * F, F * F), take[...])
    for s in range(SLOTS // 2):
        low, high = rims[s * F : (s + 1) * F], rims[(s + 2) * F : (s + 3) * F]
        c_send[s] = jnp.where(lane_f < 64, low, high)

    def c_copy(o):
        return x_copy(2, o, c_send, c_buf.at[ix])

    run_if(iz == 1, nx, [c_copy])
    f_buf[ix] = p_own[...]
    m_buf[ix] = m_send[...]
    c_buf[ix] = c_send[...]
    z_copy.wait()
    own[...] += z_recv[...]

    def w_copy(o):
        return y_copy(0, o, own, own)

    run(ny, [w_copy], "start")
    run_if(iz == 0, nx, [m_copy, c_copy])

    homes = [pick(dev == (t * ny + iy) * nz + iz, home) for t in range(nx)]

    def brick_plan(t):
        here = brick == (ix * ny + t) * nz + iz
        held = [pick(here & (box == j), slot) for j in range(SLOTS)]
        low = pick(here & (box == 0), near_slot[0])
        high = pick(here & (box == SLOTS - 1), near_slot[1])
        near = [(held[j - 1] if j > 0 else low, held[j + 1] if j < SLOTS - 1 else high) for j in range(SLOTS)]
        return [jnp.maximum(n, 0) for n in held], near

    bricks = [brick_plan(t) for t in range(ny)]
    own_held, own_near = brick_plan(iy)

    side_x = SLOTS * nz * ny
    sources = []
    for t in range(ny):
        there = dev == (ix * ny + t) * nz + iz
        codes = []
        for i in range(IFACES):
            code = jnp.where(there & (box == i), far_dev[0], jnp.where(there & (box == i - 1), far_dev[1], -1))
            codes.append(lax.div(jnp.maximum(jnp.max(code), 0), nz * ny))
        sources.append(codes)
    run(nx, [f_copy], "wait")
    for t in range(ny):
        held, near = bricks[t]
        for j in range(SLOTS):
            tx = lax.div(held[j], side_x)
            for side in range(2):
                other = lax.div(jnp.maximum(near[j][side], 0), side_x)
                if side == 0:
                    at = j if j > 0 else SLOTS
                else:
                    at = j + 1 if j < SLOTS - 1 else 0
                qf_send[t, 2 * j + side, 0:3] = f_buf[other, at, 0:3]
                qf_send[t, 2 * j + side, 3:4] = f_buf[tx, j + side, 3:4]
        for i in range(IFACES):
            at = SLOTS if i == 0 else (0 if i == SLOTS else i)
            for k in range(3):
                n = 3 * i + k
                qf_send[t, 2 * SLOTS + n // 4, n % 4 : n % 4 + 1] = f_buf[sources[t][i], at, k : k + 1]
        qf_send[t, FACES - 1, 3:4] = jnp.zeros((1, F * F), jnp.float32)
    qf_buf[iy] = qf_send[iy]

    def qf_copy(o):
        return y_copy(3, o, qf_send.at[y_peer(o)], qf_buf.at[iy])

    run(ny, [qf_copy], "start")

    run(ny, [w_copy], "wait")
    lines_load.wait()
    low_line = rem(line_id, 2) == 0
    target_home = [jnp.maximum(h, 0) for h in homes]
    target_x = [lax.div(h, ny) for h in target_home] + [ix]
    target_y = [lax.rem(h, ny) for h in target_home] + [iy]
    mixed = []
    for hy in target_y:
        before, after = jnp.maximum(hy - 1, 0), jnp.minimum(hy + 1, ny - 1)
        low_on, high_on = as_float(hy > 0), as_float(hy < ny - 1)
        for first, last in ((bx, edge_at), (line_at, line_at + 2)):
            low, high = w_buf[before, first:last] * low_on, w_buf[after, first:last] * high_on
            mixed.append(jnp.where(low_line, low, high))
        mixed.append(jnp.zeros((6, LANES), jnp.float32))
    extras = exact_right(jnp.concatenate(mixed, axis=0), lines[...])

    def assemble(n):
        hy = target_y[n]
        extra = extras[n * (half + 8) : (n + 1) * (half + 8)]
        base = w_buf[hy]
        main = (base[0:half] + extra[0:half, 0:LANES], base[half:bx] + extra[0:half, LANES : 2 * LANES])
        ends = base[edge_at : edge_at + 2] + extra[half : half + 2, 0:LANES]
        inner, outer = {}, {}
        for k in range(3):
            for side in range(2):
                at = inner_at + 2 * k + side
                first = (2 + 2 * k + side) * LANES
                from_row = 0 if side == 0 else half - 1
                inner[k, side] = base[at : at + 1] + extra[from_row : from_row + 1, first : first + LANES]
                first = (2 + 2 * k) * LANES
                outer[k, side] = base[at + 6 : at + 7] + extra[half + side : half + side + 1, first : first + LANES]
        return main, ends, inner, outer

    home_main, home_ends, home_inner, home_outer = assemble(nx)
    for t in range(nx):
        main, ends, inner, outer = assemble(t)
        d = target_x[t] - ix
        same, up_one, down_one = as_float(d == 0), as_float(d == 1), as_float(d == -1)
        e_send[t, 0:half] = main[0] * same
        e_send[t, half:bx] = main[1] * same
        e_send[t, bx : bx + 1] = ends[0:1] * up_one
        e_send[t, bx + 1 : bx + 2] = ends[1:2] * down_one
        for k in range(3):
            for side in range(2):
                at = bx + 2 + 2 * k + side
                e_send[t, at : at + 1] = inner[k, side] * (0.25 * same) + outer[k, side] * (
                    0.75 * (down_one if side else up_one)
                )
        above = ix < t
        at = bx + 8
        e_send[t, at : at + 1] = jnp.where(above, home_ends[0:1], home_ends[1:2])
        for k in range(3):
            e_send[t, at + 1 + k : at + 2 + k] = 0.75 * jnp.where(above, home_outer[k, 0], home_outer[k, 1])
    e_buf[ix] = e_send[ix]

    def e_copy(o):
        return x_copy(3, o, e_send.at[x_peer(o)], e_buf.at[ix])

    run(nx, [e_copy], "start")

    run(nx, [m_copy, c_copy], "wait")
    for t in range(ny):
        held = bricks[t][0]
        for j in range(SLOTS):
            n = held[j]
            tx, s = lax.div(n, side_x), lax.rem(n, SLOTS)
            qm_send[t, j] = m_buf[tx, s]
            rim = c_buf[tx, lax.rem(s, 2)]
            flip = lax.div(s, 2) != j // 2
            rim = jnp.where(flip, pltpu.roll(rim, 64, 1), rim)
            keep = lane_f < 64 if j < 2 else lane_f >= 64
            if j < 2:
                qc_send[t, j] = rim
            else:
                qc_send[t, j % 2] = jnp.where(keep, rim, qc_send[t, j % 2])
    qm_buf[iy] = qm_send[iy]
    qc_buf[iy] = qc_send[iy]

    def qm_copy(o):
        return y_copy(1, o, qm_send.at[y_peer(o)], qm_buf.at[iy])

    def qc_copy(o):
        return y_copy(2, o, qc_send.at[y_peer(o)], qc_buf.at[iy])

    run(ny, [qc_copy, qm_copy], "start")

    def blended(boxes_of):
        shape = (SLOTS * F, bx + 8)
        out_line = lax.broadcasted_iota(jnp.int32, shape, 0)
        from_line = lax.broadcasted_iota(jnp.int32, shape, 1)
        boxes = jnp.full(shape, boxes_of[0], jnp.int32)
        for s in range(1, SLOTS):
            boxes = jnp.where(out_line // F == s, boxes_of[s], boxes)
        f_id = out_line % F
        center = B * boxes + f_id // 2
        other = jnp.where(f_id % 2 == 0, center - 1, center + 1)
        other = jnp.where(other < 0, bx, jnp.where(other >= bx, bx + 1, other))
        return jnp.where(from_line == center, 0.75, jnp.where(from_line == other, 0.25, 0.0))

    blend = blended([slots[s][1] for s in range(SLOTS)])
    home_blend = blended(list(range(SLOTS)))
    for load in (ghost_load, rim_ghost_load, rim_mean_load):
        load.wait()
    run(nx, [e_copy], "wait")
    run(ny, [qf_copy], "wait")
    total = e_buf[0, 0 : bx + 8]
    for t in range(1, nx):
        total += e_buf[t, 0 : bx + 8]
    along = exact_left(blend, total)
    ghosts = exact_right(along, ghost[:, 0 : 3 * F * F])
    faces = exact_right(total[bx : bx + 8], ghost[:, 3 * F * F :])
    for s in range(SLOTS):
        active, b, near = slots[s]
        cv = step_rate * visc[s]
        for k in range(3):
            ends = []
            for side in range(2):
                has, is_local, _, sy = near[side]
                n = 3 * (b + side) + k
                far = qf_buf[sy, 2 * SLOTS + lax.div(n, 4), pl.ds(lax.rem(n, 4), 1)]
                outer = faces[2 + 2 * k + side : 3 + 2 * k + side]
                ends.append(jnp.where(has, far * as_float(~is_local), outer))
            edge = jnp.where(row == 0, ends[0], jnp.where(row == F - 1, ends[1], 0.0))
            at = (s * 3 + k) * F
            ghost_k = ghosts[s * F : s * F + F, k * F * F : (k + 1) * F * F]
            adv = jnp.concatenate([advs[0, at : at + F], advs[1, at : at + F]], axis=1) + cv * (ghost_k + edge)
            fine_out[k, s] = jnp.where(active, adv, 0.0)

    before = e_buf[jnp.maximum(ix - 1, 0), bx + 8 : E_ROWS] * as_float(ix > 0)
    after = e_buf[jnp.minimum(ix + 1, nx - 1), bx + 8 : E_ROWS] * as_float(ix < nx - 1)
    face_lines = []
    for k in range(3):
        for side in range(2):
            far = after if side else before
            face_lines.append(0.25 * home_inner[k, side] + far[1 + k : 2 + k])
    home_total = jnp.concatenate([*home_main, before[0:1], after[0:1], *face_lines], axis=0)
    home_along = exact_left(home_blend, home_total)
    rim_ghosts = exact_right(home_along, rim_ghost[...])
    home_faces = exact_right(home_total[bx : bx + 8], ghost[:, 3 * F * F :])
    run(ny, [qc_copy, qm_copy], "wait")

    def row_of(n):
        return lax.rem(lax.div(jnp.maximum(n, 0), SLOTS * nz), ny)

    x_lines = []
    for j in range(SLOTS):
        own_row = row_of(own_held[j])
        own_dev = lax.div(own_held[j], SLOTS)
        for side in range(2):
            m = own_near[j][side]
            other_dev = lax.div(jnp.maximum(m, 0), SLOTS)
            on = as_float((m < 0) | (own_dev != other_dev))
            weight = qf_buf[own_row, 2 * j + side, 3:4] * on
            for k in range(3):
                far = qf_buf[row_of(m), 2 * j + side, k : k + 1]
                x_lines.append(weight * jnp.where(m >= 0, far, home_faces[2 + 2 * k + side : 3 + 2 * k + side]))
    x_means = exact_right(jnp.concatenate(x_lines, axis=0), mean[...])
    products = []
    for j in range(SLOTS // 2):
        low = qc_buf[row_of(own_held[j]), j]
        high = qc_buf[row_of(own_held[j + 2]), j]
        rim = jnp.where(lane_f < 64, low, high)
        for k in range(3):
            low = rim_ghosts[j * F : (j + 1) * F, k * LANES : (k + 1) * LANES]
            high = rim_ghosts[(j + 2) * F : (j + 3) * F, k * LANES : (k + 1) * LANES]
            window[(3 * j + k) // 2, (3 * j + k) % 2 * F : (3 * j + k) % 2 * F + F] = rim * jnp.where(
                lane_f < 64, low, high
            )
    for n in range(3):
        products.append(window[n, pl.ds(0, F, 2)] + window[n, pl.ds(1, F, 2)])
    rim_means = exact_right(jnp.concatenate(products, axis=0), rim_mean[...])
    for j in range(SLOTS):
        own_row = row_of(own_held[j])
        for k in range(3):
            at = (3 * (j % 2) + k) * B
            low, high = rim_means[at : at + quarter], rim_means[at + quarter : at + B]
            if j < 2:
                high = pltpu.roll(high, 64, 1)
            else:
                low = pltpu.roll(low, 64, 1)
            value = qm_buf[own_row, j, k * quarter : (k + 1) * quarter] + jnp.where(lane_m < 64, low, high)
            row_m = lax.broadcasted_iota(jnp.int32, (quarter, LANES), 0)
            for side in range(2):
                n = (2 * j + side) * 3 + k
                place = (row_m == 0) & (lane_m < 64) if side == 0 else (row_m == quarter - 1) & (lane_m >= 64)
                value += jnp.where(place, x_means[n : n + 1], 0.0)
            picked[j, k * quarter : (k + 1) * quarter] = value


def final_kernel(dims, corners, slot_ref, field, picked, fine, coarse_out, fine_out, group, sems):
    nx, ny, nz, bx, by, bz = dims
    ix, iy, iz = lax.axis_index("gx"), lax.axis_index("gy"), lax.axis_index("gz")
    me = (ix * ny + iy) * nz + iz
    fine_copy = pltpu.make_async_copy(fine, fine_out, sems.at[0, 0])
    fine_copy.start()
    _, _, _, brick, place = grid_tables((bx, by, bz), ny, nz, corners, slot_ref)
    code = pick(brick == me, place)
    present = code >= 0
    code = jnp.maximum(code, 0)
    y_group = lax.div(lax.div(code, bz), B)
    z = lax.rem(code, bz)
    tiles = bz // LANES
    low = lax.rem(z, LANES)
    tile = lax.div(z, LANES)
    def at(g, t):
        return coarse_out.at[:, pl.ds(pl.multiple_of(g * B, B), B), pl.ds(pl.multiple_of(t * LANES, LANES), LANES)]

    def plain(g, t):
        return pltpu.make_async_copy(field.at[t, :, g * B : (g + 1) * B], at(g, t), sems.at[1 + g, t])

    def patched(g, t):
        return pltpu.make_async_copy(group, at(g, t), sems.at[1 + g, t])

    for g in range(by // B):
        for t in range(tiles):

            @pl.when((y_group != g) | (tile != t))
            def _():
                plain(g, t).start()

    start = pl.multiple_of(y_group * B, B)
    lane = lax.broadcasted_iota(jnp.int32, (B, LANES), 1)
    eight = lane // B
    line = lax.broadcasted_iota(jnp.int32, (B, LANES), 0)
    chosen = eight % B == line
    first_half = (eight - line + 16) % 16 < B
    inside = (lane >= low) & (lane < low + B) & present
    for j in range(SLOTS):
        for row in range(MEAN_ROWS):
            value = jnp.where(chosen, jnp.broadcast_to(picked[j, row : row + 1], (B, LANES)), 0.0)
            for step in (B, 2 * B, 4 * B):
                value += pltpu.roll(value, step, 1)
            swapped = pltpu.roll(value, 64, 1)
            k, a = row // (B // 2), row % (B // 2)
            for h in range(2):
                new = jnp.where(first_half, value, swapped) if h == 0 else jnp.where(first_half, swapped, value)
                x = k * bx + j * B + h * (B // 2) + a
                group[x] = jnp.where(inside, new, field[tile, x, pl.ds(start, B)])
    patched(y_group, tile).start()
    for g in range(by // B):
        for t in range(tiles):
            patched(g, t).wait()
    fine_copy.wait()


def on_device(coarse_field, fine_field, viscosity, corners, grid_slot, neighbors):
    nx, ny, nz = (lax.axis_size(n) for n in ("gx", "gy", "gz"))
    assert nz == 2
    bx, by, bz = coarse_field.shape[1:]
    dims = (nx, ny, nz, bx, by, bz)
    consts = matrices()
    vmem = pl.BlockSpec(memory_space=pltpu.VMEM)
    hbm = pl.BlockSpec(memory_space=pltpu.HBM)
    stay = functools.partial(pltpu.with_memory_space_constraint, memory_space=pltpu.HBM)
    grids = grid_slot.shape[0]
    f32 = jnp.float32
    dma = pltpu.SemaphoreType.DMA
    w_rows = bx + bx // 2 + 16
    planes = (IFACES, PLANE_LINES, F * F)
    means = (SLOTS, MEAN_ROWS, LANES)
    rims = (SLOTS // 2, F, LANES)
    tables_in = (corners.T, grid_slot.reshape(1, -1))
    fine_new, picked, field = pl.pallas_call(
        functools.partial(step_kernel, dims),
        out_shape=(
            jax.ShapeDtypeStruct(fine_field.shape, f32),
            jax.ShapeDtypeStruct((SLOTS, MEAN_ROWS, LANES), f32),
            jax.ShapeDtypeStruct((bz // LANES, 3 * bx, by + 8, LANES), f32),
        ),
        in_specs=[hbm] * (6 + len(consts)),
        out_specs=(vmem, vmem, vmem),
        scratch_shapes=[
            pltpu.VMEM((3, grids), jnp.int32),
            pltpu.VMEM((1, grids), jnp.int32),
            pltpu.VMEM((2, grids), jnp.int32),
            pltpu.VMEM(fine_field.shape, f32),
            pltpu.VMEM(viscosity.shape, f32),
        ]
        + [pltpu.VMEM(c.shape, c.dtype) for c in consts]
        + [
            pltpu.VMEM(shape, f32)
            for shape in (
                (3, bx + 8, LANES),
                (w_rows, LANES),
                (w_rows, LANES),
                (ny, w_rows, LANES),
                planes,
                (nx, *planes),
                (nx, E_ROWS, LANES),
                (nx, E_ROWS, LANES),
                (2, 3 * SLOTS * F, LANES),
                means,
                (nx, *means),
                rims,
                (nx, *rims),
                (ny, *means),
                (ny, *means),
                (ny, *rims),
                (ny, *rims),
                (ny, FACES, PLANE_LINES, F * F),
                (ny, FACES, PLANE_LINES, F * F),
            )
        ]
        + [
            dma((12 + bz // LANES,)),
            dma((2,)),
            dma((4, ny - 1)),
            dma((4, ny - 1)),
            dma((4, nx - 1)),
            dma((4, nx - 1)),
        ],
        compiler_params=pltpu.CompilerParams(collective_id=0, has_side_effects=True, vmem_limit_bytes=24 * MIB),
        name="step",
    )(
        *map(
            stay, (*tables_in, neighbors.T, coarse_field.reshape(3 * bx, by, bz), fine_field, viscosity, *consts)
        )
    )
    coarse_out, fine_out = pl.pallas_call(
        functools.partial(final_kernel, dims),
        out_shape=(
            jax.ShapeDtypeStruct((3 * bx, by, bz), f32),
            jax.ShapeDtypeStruct(fine_field.shape, f32),
        ),
        in_specs=[vmem] * 5,
        out_specs=(hbm, hbm),
        scratch_shapes=[pltpu.VMEM((3 * bx, B, LANES), f32), dma((1 + by // B, bz // LANES))],
        compiler_params=pltpu.CompilerParams(vmem_limit_bytes=16 * MIB),
        name="final",
    )(*tables_in, field, picked, fine_new)
    return fine_out, coarse_out.reshape(coarse_field.shape)


def solution(mesh):
    in_specs = (
        P(None, "gx", "gy", "gz"),
        P(None, ("gx", "gy", "gz"), None, None),
        P(("gx", "gy", "gz"), None, None),
        P(),
        P(),
        P(),
    )
    out_specs = (P(None, ("gx", "gy", "gz"), None, None), P(None, "gx", "gy", "gz"))
    return jax.shard_map(
        on_device, mesh=mesh, in_specs=in_specs, out_specs=out_specs, check_vma=False
    )
```

```python
import functools
import numpy as np
import jax
import jax.numpy as jnp
from jax import lax
from jax.experimental import pallas as pl
from jax.experimental.pallas import tpu as pltpu
from jax.sharding import PartitionSpec as P

B = 8
F = 16
SLOTS = 4
SIDE = B + 2
LANES = 128
WIDE = 4 * SIDE
IFACES = SLOTS + 1
PLANE_LINES = 4
FACES = 12
E_ROWS = 44
MEAN_ROWS = 12
step_rate = 0.15
MIB = 1 << 20


def tables():
    tangent = np.zeros((F, SIDE), np.float32)
    for f in range(F):
        c = f // 2 + 1
        tangent[f, c] = 0.75
        tangent[f, c - 1 if f % 2 == 0 else c + 1] = 0.25
    low = np.zeros((SIDE,), np.float32)
    low[0], low[1] = 0.75, 0.25
    return tangent, low, low[::-1].copy()


def matrices():
    tangent, low, high = tables()
    eye = np.eye(SIDE, dtype=np.float32)
    cut = np.zeros((SIDE, SIDE, 4, SIDE), np.float32)
    cut[:, :, 0] = np.einsum("b,cd->bcd", low, eye)
    cut[:, :, 1] = np.einsum("b,cd->bcd", high, eye)
    cut[:, :, 2] = np.einsum("bd,c->bcd", eye, low)
    cut[:, :, 3] = np.einsum("bd,c->bcd", eye, high)
    put = np.zeros((4, SIDE, F, F), np.float32)
    put[0, :, 0, :] = tangent.T
    put[1, :, F - 1, :] = tangent.T
    put[2, :, :, 0] = tangent.T
    put[3, :, :, F - 1] = tangent.T
    columns = np.zeros((3, LANES, LANES), np.float32)
    lines = np.zeros((LANES, 8, LANES), np.float32)
    ghost = np.zeros((LANES, 4, F * F), np.float32)
    for k in range(3):
        columns[k, : SIDE * SIDE, k * WIDE : (k + 1) * WIDE] = cut.reshape(SIDE * SIDE, WIDE)
        ghost[k * WIDE : (k + 1) * WIDE, k] = put.reshape(WIDE, F * F)
        for half in range(2):
            for side in range(2):
                for c in range(SIDE):
                    lane = half * 64 + k * 2 * SIDE + side * SIDE + c
                    window = side * (SIDE - 1) * SIDE + c
                    lines[lane, half] = columns[k, window]
                    lines[lane, 2 + 2 * k + half, window] = 1.0
    ghost[: SIDE * SIDE, 3] = np.einsum("sb,tc->bcst", tangent, tangent).reshape(SIDE * SIDE, F * F)
    mean = np.zeros((F * F, LANES), np.float32)
    for y in range(F):
        for z in range(F):
            for half in range(2):
                mean[y * F + z, half * 64 + (y // 2) * B + z // 2] = 0.125
    rim = [y * F + z for y in range(F) for z in range(F) if y in (0, F - 1) or z in (0, F - 1)]
    take = np.zeros((F * F, LANES), np.float32)
    rim_ghost = np.zeros((LANES, 3, LANES), np.float32)
    rim_mean = np.zeros((LANES, LANES), np.float32)
    for m, at in enumerate(rim):
        for half in range(2):
            take[at, half * 64 + m] = 1.0
            rim_ghost[:, :, half * 64 + m] = ghost[:, :3, at]
            rim_mean[half * 64 + m, half * 64 + (at // F // 2) * B + at % F // 2] = 0.125
    def twice(a):
        a = a.reshape(LANES, -1)
        return np.concatenate([a, a], axis=0)

    shapes = (
        np.concatenate([twice(a) for a in columns], axis=0), twice(lines), twice(ghost),
        mean, take, twice(rim_ghost), twice(rim_mean),
    )
    return tuple(jnp.asarray(a, jnp.bfloat16) for a in shapes)


def div(a, n):
    return lax.div(a, jnp.full_like(a, n))


def rem(a, n):
    return lax.rem(a, jnp.full_like(a, n))


def split(a):
    high = a.astype(jnp.bfloat16)
    return high, (a - high.astype(jnp.float32)).astype(jnp.bfloat16)


def dot(a, b):
    return jnp.dot(a, b, preferred_element_type=jnp.float32)


def exact_right(a, b):
    high, low = split(a)
    if b.shape[0] == 2 * a.shape[1]:
        return dot(jnp.concatenate([high, low], axis=1), b)
    return dot(high, b) + dot(low, b)


def exact_left(a, b):
    a = a.astype(jnp.bfloat16)
    high, low = split(b)
    return dot(a, high) + dot(a, low)


def pick(mask, value):
    return jnp.max(jnp.where(mask, value, -1))


def as_float(cond):
    return jnp.where(cond, 1.0, 0.0).astype(jnp.float32)


def grid_tables(bricks, ny, nz, corners, slot_ref):
    x, y, z = corners[0:1, :], corners[1:2, :], corners[2:3, :]
    slot = slot_ref[...]
    brick = (div(x, bricks[0]) * ny + div(y, bricks[1])) * nz + div(z, bricks[2])
    place = rem(y, bricks[1]) * bricks[2] + rem(z, bricks[2])
    return x, y, slot, brick, place


def step_kernel(
    dims, corners_in, slot_in, near_in, coarse, fine_in, visc_in,
    columns_in, lines_in, ghost_in, mean_in, take_in, rim_ghost_in, rim_mean_in,
    fine_out, picked, field,
    corners, slot_ref, near_ref, fine, visc, columns, lines, ghost, mean, take, rim_ghost, rim_mean,
    window, z_send, z_recv, w_buf, p_own, f_buf, e_send, e_buf,
    advs, m_send, m_buf, c_send, c_buf, qm_send, qm_buf, qc_send, qc_buf, qf_send, qf_buf,
    local_sem, z_sem, y_send_sem, y_recv_sem, x_send_sem, x_recv_sem,
):
    nx, ny, nz, bx, by, bz = dims
    ix, iy, iz = lax.axis_index("gx"), lax.axis_index("gy"), lax.axis_index("gz")
    me = (ix * ny + iy) * nz + iz
    mesh_id = pl.DeviceIdType.MESH
    tiles = bz // LANES
    half = bx // 2
    pitch = by + 8

    pairs = [
        (corners_in, corners), (slot_in, slot_ref), (near_in, near_ref), (fine_in, fine), (visc_in, visc),
        (mean_in, mean), (take_in, take),
    ]
    for t in range(tiles):
        pairs.append((coarse.at[:, :, t * LANES : (t + 1) * LANES], field.at[t, :, 0:by]))
    pairs += [
        (columns_in, columns), (lines_in, lines), (ghost_in, ghost),
        (rim_ghost_in, rim_ghost), (rim_mean_in, rim_mean),
    ]
    loads = [pltpu.make_async_copy(src, dst, local_sem.at[i]) for i, (src, dst) in enumerate(pairs)]
    for load in loads:
        load.start()
    table_loads, field_loads = loads[:3], loads[7 : 7 + tiles]
    fine_load, visc_load, mean_load, take_load = loads[3:7]
    columns_load, lines_load, ghost_load, rim_ghost_load, rim_mean_load = loads[7 + tiles :]

    def y_peer(o):
        return lax.rem(iy + o, ny)

    def x_peer(o):
        return lax.rem(ix + o, nx)

    barrier = pltpu.get_barrier_semaphore()
    pl.semaphore_signal(barrier, inc=1, device_id={"gz": 1 - iz}, device_id_type=mesh_id)

    def greet_y(o, c):
        pl.semaphore_signal(barrier, inc=1, device_id={"gy": y_peer(o)}, device_id_type=mesh_id)
        return c

    def greet_x(o, c):
        pl.semaphore_signal(barrier, inc=1, device_id={"gx": x_peer(o)}, device_id_type=mesh_id)
        return c

    lax.fori_loop(1, ny, greet_y, 0)
    lax.fori_loop(1, nx, greet_x, 0)

    def y_copy(which, o, src, dst):
        return pltpu.make_async_remote_copy(
            src_ref=src, dst_ref=dst, send_sem=y_send_sem.at[which, o - 1], recv_sem=y_recv_sem.at[which, o - 1],
            device_id={"gy": y_peer(o)}, device_id_type=mesh_id,
        )

    def x_copy(which, o, src, dst):
        return pltpu.make_async_remote_copy(
            src_ref=src, dst_ref=dst, send_sem=x_send_sem.at[which, o - 1], recv_sem=x_recv_sem.at[which, o - 1],
            device_id={"gx": x_peer(o)}, device_id_type=mesh_id,
        )

    def run(count, makes, action):
        def body(o, c):
            for make in makes:
                getattr(make(o), action)()
            return c

        lax.fori_loop(1, count, body, 0)

    def run_if(cond, count, makes):
        @pl.when(cond)
        def _():
            run(count, makes, "start")

    for load in table_loads:
        load.wait()
    gx_, gy_, slot, brick, place = grid_tables((bx, by, bz), ny, nz, corners, slot_ref)
    home = div(gx_, bx) * ny + div(gy_, by)
    box = div(rem(gx_, bx), B)
    dev = div(slot, SLOTS)
    count = slot.shape[1]
    g_row = lax.broadcasted_iota(jnp.int32, (count, count), 0)
    g_col = lax.broadcasted_iota(jnp.int32, (count, count), 1)
    slot_col = jnp.max(jnp.where(g_row == g_col, slot, -1), axis=1, keepdims=True)
    near_slot = []
    far_dev = []
    for side in range(2):
        m = jnp.max(jnp.where(g_row == near_ref[side : side + 1, :], slot_col, -1), axis=0, keepdims=True)
        near_slot.append(m)
        d = div(jnp.maximum(m, 0), SLOTS)
        far_dev.append(jnp.where((m >= 0) & (d != dev), d, -1))

    def anchor(ox, oy, gz):
        hx, hy = ix + ox, iy + oy
        inside = (hx >= 0) & (hx < nx) & (hy >= 0) & (hy < ny)
        code = jnp.maximum(pick(brick == jnp.where(inside, (hx * ny + hy) * nz + gz, -5), place), 0)
        return lax.div(code, bz), lax.rem(code, bz)

    mine = dev == me
    own_slot = [pick(mine & (box == j), rem(slot, SLOTS)) for j in range(SLOTS)]
    slots = []
    for s in range(SLOTS):
        here = slot == me * SLOTS + s
        b = pick(here, box)
        near = []
        for side in range(2):
            m = pick(here, near_slot[side])
            n = jnp.maximum(m, 0)
            d = lax.div(n, SLOTS)
            near.append((m >= 0, d == me, lax.rem(n, SLOTS), lax.rem(lax.div(d, nz), ny)))
        slots.append((b >= 0, jnp.maximum(b, 0), near))

    fine_load.wait()
    visc_load.wait()
    for i in range(IFACES):
        below = jnp.maximum(own_slot[max(i - 1, 0)], 0)
        above = jnp.maximum(own_slot[min(i, SLOTS - 1)], 0)
        for k in range(PLANE_LINES):
            def line(n, x):
                return fine[k, n, x : x + 1] if k < 3 else step_rate * visc[n, x : x + 1]

            if i == 0:
                value = line(above, 0)
            elif i == SLOTS:
                value = line(below, F - 1)
            else:
                value = jnp.where(own_slot[i - 1] >= 0, line(below, F - 1), line(above, 0))
            p_own[i, k : k + 1] = value

    def f_copy(o):
        return x_copy(0, o, p_own, f_buf.at[ix])


    lane = lax.broadcasted_iota(jnp.int32, (F, F * F), 1)
    row = lax.broadcasted_iota(jnp.int32, (F, F * F), 0)
    lz = lane % F
    for s in range(SLOTS):
        cv = step_rate * visc[s]
        for k in range(3):
            v = fine[k, s]
            ends = []
            for side in range(2):
                has, is_local, n, _ = slots[s][2][side]
                x = (F - 1) * (1 - side)
                ends.append(fine[k, n][x : x + 1] * as_float(has & is_local))
            total = jnp.where(row == 0, ends[0], pltpu.roll(v, 1, 0))
            total += jnp.where(row == F - 1, ends[1], pltpu.roll(v, F - 1, 0))
            total += jnp.where(lane < F, 0.0, pltpu.roll(v, F, 1))
            total += jnp.where(lane >= F * F - F, 0.0, pltpu.roll(v, F * F - F, 1))
            total += jnp.where(lz == 0, 0.0, pltpu.roll(v, 1, 1))
            total += jnp.where(lz == F - 1, 0.0, pltpu.roll(v, F * F - 1, 1))
            at = (s * 3 + k) * F
            value = v + cv * (total - 6.0 * v)
            advs[0, at : at + F] = value[:, :LANES]
            advs[1, at : at + F] = value[:, LANES:]
    rows = 3 * SLOTS * F // 2
    mean_load.wait()
    sums = [advs[h, pl.ds(0, rows, 2)] + advs[h, pl.ds(1, rows, 2)] for h in range(2)]
    z = exact_right(jnp.concatenate(sums, axis=1), mean[...])
    quarter = B // 2
    lane_m = lax.broadcasted_iota(jnp.int32, (quarter, LANES), 1)
    for s in range(SLOTS):
        for k in range(3):
            at = (s * 3 + k) * B
            m_send[s, k * quarter : (k + 1) * quarter] = jnp.where(
                lane_m < 64, z[at : at + quarter], z[at + quarter : at + B]
            )
    def m_copy(o):
        return x_copy(1, o, m_send, m_buf.at[ix])

    pl.semaphore_wait(barrier, nx + ny - 1)
    run(nx, [f_copy], "start")
    run_if(iz == 1, nx, [m_copy])

    anchors = [
        {(ox, oy): anchor(ox, oy, gz) for ox in (-1, 0, 1) for oy in (-1, 0, 1)} for gz in (1 - iz, iz)
    ]
    flat = field.reshape(tiles, 3 * bx * pitch, LANES)
    stride = bx * pitch
    lane1 = lax.broadcasted_iota(jnp.int32, (1, LANES), 1)
    lane_b = div(lane1, SIDE)
    lane_c = rem(lane1, SIDE)
    half_lane = rem(lane1, 64)
    half_c = rem(half_lane, SIDE)
    line_id = div(half_lane, SIDE)

    def shifted(z, same, start, size, step, to):
        def get(t):
            return flat[t, pl.ds(start, size, step)] if size > 1 else flat[t, pl.ds(start, 1)]

        z = lax.rem(z - 1 + bz, bz)
        tile, low = lax.div(z, LANES), lax.rem(z, LANES)
        if same:
            lane = lax.broadcasted_iota(jnp.int32, (size, LANES), 1)
            value = jnp.where(lane >= low, get(tile), get(lax.rem(tile + 1, tiles)))
        else:
            value = get((tiles - 1) * (1 - iz))
        return pltpu.roll(value, lax.rem(to - low + LANES, LANES), 1)

    def z_weight(z, ids, same):
        first, last = z == 0, z == bz - B
        if same:
            return jnp.where(ids == 0, as_float(~first), jnp.where(ids == SIDE - 1, as_float(~last), 1.0))
        first = as_float(first & (iz == 0))
        last = as_float(last & (iz == 1))
        return jnp.where(ids == 0, first, jnp.where(ids == SIDE - 1, last, 0.0))

    def weights(y, z, same):
        weight = z_weight(z, lane_c, same)
        weight = weight * jnp.where(
            lane_b == 0, as_float(y > 0), jnp.where(lane_b == SIDE - 1, as_float(y < by - B), 1.0)
        )
        return jnp.where(lane1 < SIDE * SIDE, weight, 0.0)

    edge_at = bx + half
    line_at = edge_at + 2
    inner_at = line_at + 2
    outer_at = inner_at + 6

    def pack(place, same, to_ref):
        y, z = place[0, 0]
        weight = weights(y, z, same)
        for k in range(3):
            acc = jnp.zeros((bx, LANES), jnp.float32)
            for b in range(SIDE):
                at = jnp.clip(y - 1 + b, 0, by - 1)
                value = shifted(z, same, k * stride + at, bx, pitch, SIDE * b)
                acc = jnp.where(lane_b == b, value, acc)
            window[k, 0:bx] = acc * weight
        for n, ox in enumerate((1, -1)):
            y, z = place[ox, 0]
            weight = weights(y, z, same)
            x = bx - 1 if ox > 0 else 0
            acc = jnp.zeros((3, LANES), jnp.float32)
            for b in range(SIDE):
                at = jnp.clip(y - 1 + b, 0, by - 1)
                acc = jnp.where(lane_b == b, shifted(z, same, x * pitch + at, 3, stride, SIDE * b), acc)
            acc = acc * weight
            for k in range(3):
                window[k, bx + n : bx + n + 1] = acc[k : k + 1]
        total = jnp.zeros((bx + 8, LANES), jnp.float32)
        for k in range(3):
            total += exact_right(window[k], columns[2 * k * LANES : 2 * (k + 1) * LANES])
            for side in range(2):
                at = inner_at + 2 * k + side
                inner = 0 if side == 0 else bx - 1
                to_ref[at : at + 1] = window[k, inner : inner + 1]
                to_ref[at + 6 : at + 7] = window[k, bx + side : bx + side + 1]
        to_ref[0:bx] = total[0:bx]
        to_ref[edge_at : edge_at + 2] = total[bx : bx + 2]
        main = [jnp.zeros((half, LANES), jnp.float32) for _ in range(2)]
        ends = [jnp.zeros((1, LANES), jnp.float32) for _ in range(2)]
        for side, oy in enumerate((1, -1)):
            at = by - 1 if oy > 0 else 0
            edge = 0 if oy > 0 else by - B
            y, z = place[0, oy]
            weight = z_weight(z, half_c, same) * as_float(y == edge)
            for k in range(3):
                to = k * 2 * SIDE + side * SIDE
                for h in range(2):
                    value = shifted(z, same, k * stride + h * half * pitch + at, half, pitch, to + 64 * h)
                    main[h] = jnp.where(line_id == 2 * k + side, value * weight, main[h])
            for n, ox in enumerate((1, -1)):
                y, z = place[ox, oy]
                weight = z_weight(z, half_c, same) * as_float(y == edge)
                x = bx - 1 if ox > 0 else 0
                for k in range(3):
                    to = k * 2 * SIDE + side * SIDE
                    value = shifted(z, same, k * stride + x * pitch + at, 1, 1, to)
                    ends[n] = jnp.where(line_id == 2 * k + side, value * weight, ends[n])
        to_ref[bx:edge_at] = jnp.where(lane1 < 64, main[0], main[1])
        for n in range(2):
            to_ref[line_at + n : line_at + n + 1] = jnp.where(lane1 < 64, ends[n], 0.0)

    own = w_buf.at[iy]
    for k in range(3):
        window[k, bx + 2 : bx + 8] = jnp.zeros((6, LANES), jnp.float32)
    for load in field_loads:
        load.wait()
    columns_load.wait()
    pack(anchors[0], False, z_send)
    z_copy = pltpu.make_async_remote_copy(
        src_ref=z_send, dst_ref=z_recv, send_sem=z_sem.at[0], recv_sem=z_sem.at[1],
        device_id={"gz": 1 - iz}, device_id_type=mesh_id,
    )
    z_copy.start()
    pack(anchors[1], True, own)
    take_load.wait()
    lane_f = lax.broadcasted_iota(jnp.int32, (F, LANES), 1)
    rims = exact_right(step_rate * visc[...].reshape(SLOTS * F, F * F), take[...])
    for s in range(SLOTS // 2):
        low, high = rims[s * F : (s + 1) * F], rims[(s + 2) * F : (s + 3) * F]
        c_send[s] = jnp.where(lane_f < 64, low, high)

    def c_copy(o):
        return x_copy(2, o, c_send, c_buf.at[ix])

    run_if(iz == 1, nx, [c_copy])
    f_buf[ix] = p_own[...]
    m_buf[ix] = m_send[...]
    c_buf[ix] = c_send[...]
    z_copy.wait()
    own[...] += z_recv[...]

    def w_copy(o):
        return y_copy(0, o, own, own)

    run(ny, [w_copy], "start")
    run_if(iz == 0, nx, [m_copy, c_copy])

    homes = [pick(dev == (t * ny + iy) * nz + iz, home) for t in range(nx)]

    def brick_plan(t):
        here = brick == (ix * ny + t) * nz + iz
        held = [pick(here & (box == j), slot) for j in range(SLOTS)]
        low = pick(here & (box == 0), near_slot[0])
        high = pick(here & (box == SLOTS - 1), near_slot[1])
        near = [(held[j - 1] if j > 0 else low, held[j + 1] if j < SLOTS - 1 else high) for j in range(SLOTS)]
        return [jnp.maximum(n, 0) for n in held], near

    bricks = [brick_plan(t) for t in range(ny)]
    own_held, own_near = brick_plan(iy)

    side_x = SLOTS * nz * ny
    sources = []
    for t in range(ny):
        there = dev == (ix * ny + t) * nz + iz
        codes = []
        for i in range(IFACES):
            code = jnp.where(there & (box == i), far_dev[0], jnp.where(there & (box == i - 1), far_dev[1], -1))
            codes.append(lax.div(jnp.maximum(jnp.max(code), 0), nz * ny))
        sources.append(codes)
    run(nx, [f_copy], "wait")
    for t in range(ny):
        held, near = bricks[t]
        for j in range(SLOTS):
            tx = lax.div(held[j], side_x)
            for side in range(2):
                other = lax.div(jnp.maximum(near[j][side], 0), side_x)
                if side == 0:
                    at = j if j > 0 else SLOTS
                else:
                    at = j + 1 if j < SLOTS - 1 else 0
                qf_send[t, 2 * j + side, 0:3] = f_buf[other, at, 0:3]
                qf_send[t, 2 * j + side, 3:4] = f_buf[tx, j + side, 3:4]
        for i in range(IFACES):
            at = SLOTS if i == 0 else (0 if i == SLOTS else i)
            for k in range(3):
                n = 3 * i + k
                qf_send[t, 2 * SLOTS + n // 4, n % 4 : n % 4 + 1] = f_buf[sources[t][i], at, k : k + 1]
        qf_send[t, FACES - 1, 3:4] = jnp.zeros((1, F * F), jnp.float32)
    qf_buf[iy] = qf_send[iy]

    def qf_copy(o):
        return y_copy(3, o, qf_send.at[y_peer(o)], qf_buf.at[iy])

    run(ny, [qf_copy], "start")

    run(ny, [w_copy], "wait")
    lines_load.wait()
    low_line = rem(line_id, 2) == 0
    target_home = [jnp.maximum(h, 0) for h in homes]
    target_x = [lax.div(h, ny) for h in target_home] + [ix]
    target_y = [lax.rem(h, ny) for h in target_home] + [iy]
    mixed, side_lines = [], []
    for hy in target_y:
        before, after = jnp.maximum(hy - 1, 0), jnp.minimum(hy + 1, ny - 1)
        low_on, high_on = as_float(hy > 0), as_float(hy < ny - 1)
        for first, last in ((bx, edge_at), (line_at, line_at + 2)):
            low, high = w_buf[before, first:last] * low_on, w_buf[after, first:last] * high_on
            mixed.append(jnp.where(low_line, low, high))
        side_lines += [mixed[-2][0:1], mixed[-2][half - 1 : half], mixed[-1]]
        mixed.append(jnp.zeros((6, LANES), jnp.float32))
    extras = exact_right(jnp.concatenate(mixed, axis=0), lines[:, 0 : 2 * LANES])
    side_lines.append(jnp.zeros((-len(target_y) * 4 % 8, LANES), jnp.float32))
    side_extras = exact_right(jnp.concatenate(side_lines, axis=0), lines[:, 2 * LANES :])

    def assemble(n):
        hy = target_y[n]
        extra = extras[n * (half + 8) : (n + 1) * (half + 8)]
        side_extra = side_extras[4 * n : 4 * n + 4]
        base = w_buf[hy]
        main = (base[0:half] + extra[0:half, 0:LANES], base[half:bx] + extra[0:half, LANES : 2 * LANES])
        ends = base[edge_at : edge_at + 2] + extra[half : half + 2, 0:LANES]
        inner, outer = {}, {}
        for k in range(3):
            for side in range(2):
                at = inner_at + 2 * k + side
                first = (2 * k + side) * LANES
                inner[k, side] = base[at : at + 1] + side_extra[side : side + 1, first : first + LANES]
                first = 2 * k * LANES
                outer[k, side] = base[at + 6 : at + 7] + side_extra[2 + side : 3 + side, first : first + LANES]
        return main, ends, inner, outer

    home_main, home_ends, home_inner, home_outer = assemble(nx)
    for t in range(nx):
        main, ends, inner, outer = assemble(t)
        d = target_x[t] - ix
        same, up_one, down_one = as_float(d == 0), as_float(d == 1), as_float(d == -1)
        e_send[t, 0:half] = main[0] * same
        e_send[t, half:bx] = main[1] * same
        e_send[t, bx : bx + 1] = ends[0:1] * up_one
        e_send[t, bx + 1 : bx + 2] = ends[1:2] * down_one
        for k in range(3):
            for side in range(2):
                at = bx + 2 + 2 * k + side
                e_send[t, at : at + 1] = inner[k, side] * (0.25 * same) + outer[k, side] * (
                    0.75 * (down_one if side else up_one)
                )
        above = ix < t
        at = bx + 8
        e_send[t, at : at + 1] = jnp.where(above, home_ends[0:1], home_ends[1:2])
        for k in range(3):
            e_send[t, at + 1 + k : at + 2 + k] = 0.75 * jnp.where(above, home_outer[k, 0], home_outer[k, 1])
    e_buf[ix] = e_send[ix]

    def e_copy(o):
        return x_copy(3, o, e_send.at[x_peer(o)], e_buf.at[ix])

    run(nx, [e_copy], "start")

    run(nx, [m_copy, c_copy], "wait")
    for t in range(ny):
        held = bricks[t][0]
        for j in range(SLOTS):
            n = held[j]
            tx, s = lax.div(n, side_x), lax.rem(n, SLOTS)
            qm_send[t, j] = m_buf[tx, s]
            rim = c_buf[tx, lax.rem(s, 2)]
            flip = lax.div(s, 2) != j // 2
            rim = jnp.where(flip, pltpu.roll(rim, 64, 1), rim)
            keep = lane_f < 64 if j < 2 else lane_f >= 64
            if j < 2:
                qc_send[t, j] = rim
            else:
                qc_send[t, j % 2] = jnp.where(keep, rim, qc_send[t, j % 2])
    qm_buf[iy] = qm_send[iy]
    qc_buf[iy] = qc_send[iy]

    def qm_copy(o):
        return y_copy(1, o, qm_send.at[y_peer(o)], qm_buf.at[iy])

    def qc_copy(o):
        return y_copy(2, o, qc_send.at[y_peer(o)], qc_buf.at[iy])

    run(ny, [qc_copy, qm_copy], "start")

    def blended(boxes_of):
        shape = (SLOTS * F, bx + 8)
        out_line = lax.broadcasted_iota(jnp.int32, shape, 0)
        from_line = lax.broadcasted_iota(jnp.int32, shape, 1)
        boxes = jnp.full(shape, boxes_of[0], jnp.int32)
        for s in range(1, SLOTS):
            boxes = jnp.where(out_line // F == s, boxes_of[s], boxes)
        f_id = out_line % F
        center = B * boxes + f_id // 2
        other = jnp.where(f_id % 2 == 0, center - 1, center + 1)
        other = jnp.where(other < 0, bx, jnp.where(other >= bx, bx + 1, other))
        return jnp.where(from_line == center, 0.75, jnp.where(from_line == other, 0.25, 0.0))

    blend = blended([slots[s][1] for s in range(SLOTS)])
    home_blend = blended(list(range(SLOTS)))
    for load in (ghost_load, rim_ghost_load, rim_mean_load):
        load.wait()
    run(nx, [e_copy], "wait")
    run(ny, [qf_copy], "wait")
    total = e_buf[0, 0 : bx + 8]
    for t in range(1, nx):
        total += e_buf[t, 0 : bx + 8]
    along = exact_left(blend, total)
    ghosts = exact_right(along, ghost[:, 0 : 3 * F * F])
    faces = exact_right(total[bx : bx + 8], ghost[:, 3 * F * F :])
    for s in range(SLOTS):
        active, b, near = slots[s]
        cv = step_rate * visc[s]
        for k in range(3):
            ends = []
            for side in range(2):
                has, is_local, _, sy = near[side]
                n = 3 * (b + side) + k
                far = qf_buf[sy, 2 * SLOTS + lax.div(n, 4), pl.ds(lax.rem(n, 4), 1)]
                outer = faces[2 + 2 * k + side : 3 + 2 * k + side]
                ends.append(jnp.where(has, far * as_float(~is_local), outer))
            edge = jnp.where(row == 0, ends[0], jnp.where(row == F - 1, ends[1], 0.0))
            at = (s * 3 + k) * F
            ghost_k = ghosts[s * F : s * F + F, k * F * F : (k + 1) * F * F]
            adv = jnp.concatenate([advs[0, at : at + F], advs[1, at : at + F]], axis=1) + cv * (ghost_k + edge)
            fine_out[k, s] = jnp.where(active, adv, 0.0)

    before = e_buf[jnp.maximum(ix - 1, 0), bx + 8 : E_ROWS] * as_float(ix > 0)
    after = e_buf[jnp.minimum(ix + 1, nx - 1), bx + 8 : E_ROWS] * as_float(ix < nx - 1)
    face_lines = []
    for k in range(3):
        for side in range(2):
            far = after if side else before
            face_lines.append(0.25 * home_inner[k, side] + far[1 + k : 2 + k])
    home_total = jnp.concatenate([*home_main, before[0:1], after[0:1], *face_lines], axis=0)
    home_along = exact_left(home_blend, home_total)
    rim_ghosts = exact_right(home_along, rim_ghost[...])
    home_faces = exact_right(home_total[bx : bx + 8], ghost[:, 3 * F * F :])
    run(ny, [qc_copy, qm_copy], "wait")

    def row_of(n):
        return lax.rem(lax.div(jnp.maximum(n, 0), SLOTS * nz), ny)

    x_lines = []
    for j in range(SLOTS):
        own_row = row_of(own_held[j])
        own_dev = lax.div(own_held[j], SLOTS)
        for side in range(2):
            m = own_near[j][side]
            other_dev = lax.div(jnp.maximum(m, 0), SLOTS)
            on = as_float((m < 0) | (own_dev != other_dev))
            weight = qf_buf[own_row, 2 * j + side, 3:4] * on
            for k in range(3):
                far = qf_buf[row_of(m), 2 * j + side, k : k + 1]
                x_lines.append(weight * jnp.where(m >= 0, far, home_faces[2 + 2 * k + side : 3 + 2 * k + side]))
    x_means = exact_right(jnp.concatenate(x_lines, axis=0), mean[...])
    products = []
    for j in range(SLOTS // 2):
        low = qc_buf[row_of(own_held[j]), j]
        high = qc_buf[row_of(own_held[j + 2]), j]
        rim = jnp.where(lane_f < 64, low, high)
        for k in range(3):
            low = rim_ghosts[j * F : (j + 1) * F, k * LANES : (k + 1) * LANES]
            high = rim_ghosts[(j + 2) * F : (j + 3) * F, k * LANES : (k + 1) * LANES]
            window[(3 * j + k) // 2, (3 * j + k) % 2 * F : (3 * j + k) % 2 * F + F] = rim * jnp.where(
                lane_f < 64, low, high
            )
    for n in range(3):
        products.append(window[n, pl.ds(0, F, 2)] + window[n, pl.ds(1, F, 2)])
    rim_means = exact_right(jnp.concatenate(products, axis=0), rim_mean[...])
    for j in range(SLOTS):
        own_row = row_of(own_held[j])
        for k in range(3):
            at = (3 * (j % 2) + k) * B
            low, high = rim_means[at : at + quarter], rim_means[at + quarter : at + B]
            if j < 2:
                high = pltpu.roll(high, 64, 1)
            else:
                low = pltpu.roll(low, 64, 1)
            value = qm_buf[own_row, j, k * quarter : (k + 1) * quarter] + jnp.where(lane_m < 64, low, high)
            row_m = lax.broadcasted_iota(jnp.int32, (quarter, LANES), 0)
            for side in range(2):
                n = (2 * j + side) * 3 + k
                place = (row_m == 0) & (lane_m < 64) if side == 0 else (row_m == quarter - 1) & (lane_m >= 64)
                value += jnp.where(place, x_means[n : n + 1], 0.0)
            picked[j, k * quarter : (k + 1) * quarter] = value


def final_kernel(dims, corners, slot_ref, field, picked, fine, coarse_out, fine_out, group, sems):
    nx, ny, nz, bx, by, bz = dims
    ix, iy, iz = lax.axis_index("gx"), lax.axis_index("gy"), lax.axis_index("gz")
    me = (ix * ny + iy) * nz + iz
    fine_copy = pltpu.make_async_copy(fine, fine_out, sems.at[0, 0])
    fine_copy.start()
    _, _, _, brick, place = grid_tables((bx, by, bz), ny, nz, corners, slot_ref)
    code = pick(brick == me, place)
    present = code >= 0
    code = jnp.maximum(code, 0)
    y_group = lax.div(lax.div(code, bz), B)
    z = lax.rem(code, bz)
    tiles = bz // LANES
    low = lax.rem(z, LANES)
    tile = lax.div(z, LANES)
    def at(g, t):
        return coarse_out.at[:, pl.ds(pl.multiple_of(g * B, B), B), pl.ds(pl.multiple_of(t * LANES, LANES), LANES)]

    def plain(g, t):
        return pltpu.make_async_copy(field.at[t, :, g * B : (g + 1) * B], at(g, t), sems.at[1 + g, t])

    def patched(g, t):
        return pltpu.make_async_copy(group, at(g, t), sems.at[1 + g, t])

    for g in range(by // B):
        for t in range(tiles):

            @pl.when((y_group != g) | (tile != t))
            def _():
                plain(g, t).start()

    start = pl.multiple_of(y_group * B, B)
    lane = lax.broadcasted_iota(jnp.int32, (B, LANES), 1)
    eight = lane // B
    line = lax.broadcasted_iota(jnp.int32, (B, LANES), 0)
    chosen = eight % B == line
    first_half = (eight - line + 16) % 16 < B
    inside = (lane >= low) & (lane < low + B) & present
    for j in range(SLOTS):
        for row in range(MEAN_ROWS):
            value = jnp.where(chosen, jnp.broadcast_to(picked[j, row : row + 1], (B, LANES)), 0.0)
            for step in (B, 2 * B, 4 * B):
                value += pltpu.roll(value, step, 1)
            swapped = pltpu.roll(value, 64, 1)
            k, a = row // (B // 2), row % (B // 2)
            for h in range(2):
                new = jnp.where(first_half, value, swapped) if h == 0 else jnp.where(first_half, swapped, value)
                x = k * bx + j * B + h * (B // 2) + a
                group[x] = jnp.where(inside, new, field[tile, x, pl.ds(start, B)])
    patched(y_group, tile).start()
    for g in range(by // B):
        for t in range(tiles):
            patched(g, t).wait()
    fine_copy.wait()


def on_device(coarse_field, fine_field, viscosity, corners, grid_slot, neighbors):
    nx, ny, nz = (lax.axis_size(n) for n in ("gx", "gy", "gz"))
    assert nz == 2
    bx, by, bz = coarse_field.shape[1:]
    dims = (nx, ny, nz, bx, by, bz)
    consts = matrices()
    vmem = pl.BlockSpec(memory_space=pltpu.VMEM)
    hbm = pl.BlockSpec(memory_space=pltpu.HBM)
    stay = functools.partial(pltpu.with_memory_space_constraint, memory_space=pltpu.HBM)
    grids = grid_slot.shape[0]
    f32 = jnp.float32
    dma = pltpu.SemaphoreType.DMA
    w_rows = bx + bx // 2 + 16
    planes = (IFACES, PLANE_LINES, F * F)
    means = (SLOTS, MEAN_ROWS, LANES)
    rims = (SLOTS // 2, F, LANES)
    tables_in = (corners.T, grid_slot.reshape(1, -1))
    fine_new, picked, field = pl.pallas_call(
        functools.partial(step_kernel, dims),
        out_shape=(
            jax.ShapeDtypeStruct(fine_field.shape, f32),
            jax.ShapeDtypeStruct((SLOTS, MEAN_ROWS, LANES), f32),
            jax.ShapeDtypeStruct((bz // LANES, 3 * bx, by + 8, LANES), f32),
        ),
        in_specs=[hbm] * (6 + len(consts)),
        out_specs=(vmem, vmem, vmem),
        scratch_shapes=[
            pltpu.VMEM((3, grids), jnp.int32),
            pltpu.VMEM((1, grids), jnp.int32),
            pltpu.VMEM((2, grids), jnp.int32),
            pltpu.VMEM(fine_field.shape, f32),
            pltpu.VMEM(viscosity.shape, f32),
        ]
        + [pltpu.VMEM(c.shape, c.dtype) for c in consts]
        + [
            pltpu.VMEM(shape, f32)
            for shape in (
                (3, bx + 8, LANES),
                (w_rows, LANES),
                (w_rows, LANES),
                (ny, w_rows, LANES),
                planes,
                (nx, *planes),
                (nx, E_ROWS, LANES),
                (nx, E_ROWS, LANES),
                (2, 3 * SLOTS * F, LANES),
                means,
                (nx, *means),
                rims,
                (nx, *rims),
                (ny, *means),
                (ny, *means),
                (ny, *rims),
                (ny, *rims),
                (ny, FACES, PLANE_LINES, F * F),
                (ny, FACES, PLANE_LINES, F * F),
            )
        ]
        + [
            dma((12 + bz // LANES,)),
            dma((2,)),
            dma((4, ny - 1)),
            dma((4, ny - 1)),
            dma((4, nx - 1)),
            dma((4, nx - 1)),
        ],
        compiler_params=pltpu.CompilerParams(collective_id=0, has_side_effects=True, vmem_limit_bytes=24 * MIB),
        name="step",
    )(
        *map(
            stay, (*tables_in, neighbors.T, coarse_field.reshape(3 * bx, by, bz), fine_field, viscosity, *consts)
        )
    )
    coarse_out, fine_out = pl.pallas_call(
        functools.partial(final_kernel, dims),
        out_shape=(
            jax.ShapeDtypeStruct((3 * bx, by, bz), f32),
            jax.ShapeDtypeStruct(fine_field.shape, f32),
        ),
        in_specs=[vmem] * 5,
        out_specs=(hbm, hbm),
        scratch_shapes=[pltpu.VMEM((3 * bx, B, LANES), f32), dma((1 + by // B, bz // LANES))],
        compiler_params=pltpu.CompilerParams(vmem_limit_bytes=16 * MIB),
        name="final",
    )(*tables_in, field, picked, fine_new)
    return fine_out, coarse_out.reshape(coarse_field.shape)


def solution(mesh):
    in_specs = (
        P(None, "gx", "gy", "gz"),
        P(None, ("gx", "gy", "gz"), None, None),
        P(("gx", "gy", "gz"), None, None),
        P(),
        P(),
        P(),
    )
    out_specs = (P(None, ("gx", "gy", "gz"), None, None), P(None, "gx", "gy", "gz"))
    return jax.shard_map(
        on_device, mesh=mesh, in_specs=in_specs, out_specs=out_specs, check_vma=False
    )
```
